32 devices in a mesh: dp: 8 (over y, x, core), ctx: 4 (over z).
Axes of the slice: x: 2, y: 2, z: 4, core: 2. Of those that a mesh axis runs over, the one named last changes fastest.
Arguments:
- tokens: bfloat16 [8, 256, 768], P('dp', 'ctx'), may hold values from -6 to 6
- qkv_weight: bfloat16 [768, 2304], P(('dp', 'ctx')), may hold values from -0.21875 to 0.21875
- out_weight: bfloat16 [768, 768], P(('dp', 'ctx')), may hold values from -0.875 to 0.875
- up_weight: bfloat16 [768, 3072], P(('dp', 'ctx')), may hold values from -0.21875 to 0.21875
- down_weight: bfloat16 [3072, 768], P(('dp', 'ctx')), may hold values from -0.109375 to 0.109375
- attn_gain: bfloat16 [768], P(('dp', 'ctx')), may hold values from 0.5 to 1.5
- attn_shift: bfloat16 [768], P(('dp', 'ctx')), may hold values from -1.5 to 1.5
- ffn_gain: bfloat16 [768], P(('dp', 'ctx')), may hold values from 0.5 to 1.5
- ffn_shift: bfloat16 [768], P(('dp', 'ctx')), may hold values from -1.5 to 1.5
- pass_embed: bfloat16 [5, 768], P(None, ('dp', 'ctx')), may hold values from -3 to 3
- segment_ids: int32 [8, 256], P('dp', 'ctx'), may hold values from 0 to 3, never falling along the last dimension, each value on 1 to 128 neighbouring positions
- cotangent: bfloat16 [8, 1280, 768], P('dp', 'ctx'), may hold values from -6 to 6
Outputs:
- activations: bfloat16 [8, 1280, 768], P('dp', 'ctx')
- input_grad: float32 [8, 256, 768], P('dp', 'ctx')
- qkv_grad: float32 [768, 2304], P(('dp', 'ctx'))
- out_grad: float32 [768, 768], P(('dp', 'ctx'))
- up_grad: float32 [768, 3072], P(('dp', 'ctx'))
- down_grad: float32 [3072, 768], P(('dp', 'ctx'))
- attn_gain_grad: float32 [768], P(('dp', 'ctx'))
- attn_shift_grad: float32 [768], P(('dp', 'ctx'))
- ffn_gain_grad: float32 [768], P(('dp', 'ctx'))
- ffn_shift_grad: float32 [768], P(('dp', 'ctx'))
- pass_embed_grad: float32 [5, 768], P(None, ('dp', 'ctx'))
The draws below stay inside these ranges and needn't reach their ends.
Inputs may be any that keep to these rules, and one draw needn't show every extreme that they name: `segment_ids`: along the positions of a sequence the document id never falls; every document spans 1 to 128 positions, and one spans exactly 128.
All inputs are finite; a program needn't handle non-finite values.
Results may differ from the reference program's by a relative error of at most 0.012.
Values may be sent and summed in bfloat16 or wider, within the bound.
A program may use at most 192 MiB of HBM per device.

```python
import math
import jax
import jax.numpy as jnp
import numpy as np
from jax import lax

D = 768
H = 12
HD = 64
FF = 3072
R = 5
TOKS = 256
DOCS = 4
SEQS = 1
SEG_MOST = 128
NSEQ = 8
N_DP = 8


def raised(values, rng, source, target, parts, factor):
    def block_of(position):
        return (jnp.arange(values.shape[position]) // (values.shape[position] // parts)).reshape((-1,) + (1,) * (values.ndim - 1 - position))

    one_side = jax.random.permutation(rng, parts)[block_of(target)]
    second = (block_of(target) + parts // 2) % parts
    return jnp.where((block_of(source) == one_side) | (block_of(source) == second), factor * values, values)


def level_of(stream_key, extent, pieces, low, top_value):
    level = 1.0
    for dim, parts in pieces:
        heights = jax.random.uniform(jax.random.fold_in(jax.random.fold_in(stream_key, 6), dim), (parts,), jnp.float32, low / len(pieces), top_value / len(pieces))
        level = level * jnp.repeat(jnp.exp(heights), extent[dim] // parts).reshape((-1,) + (1,) * (len(extent) - 1 - dim))
    return level


def split_up(amount, total, reach, slope):
    portions = [(1 << 20) // math.isqrt(rank ** slope) + 1 for rank in range(2, amount + 1)]
    rest, holding = total - reach - (amount - 1), [1] * (amount - 1)
    while rest > 0:
        candidates = [i for i in range(amount - 1) if holding[i] < reach]
        mass, left = sum([portions[i] for i in candidates]), rest
        for i in candidates:
            extra = min(reach - holding[i], max(1, left * portions[i] // mass), rest)
            holding[i] = holding[i] + extra
            rest = rest - extra
    return np.array([reach] + holding)


def uneven(rng, count, total, limit, slope):
    if count == 2:
        one = jax.random.randint(rng, (), max(1, total - limit), min(limit, total - 1) + 1)
        return jnp.stack([one, total - one])
    sizes = jnp.asarray(split_up(count, total, limit, slope), jnp.int32)
    couples = (count - 1) // 2
    source_of, receiver = sizes[1:1 + 2 * couples:2], sizes[2:2 + 2 * couples:2]
    room = jnp.minimum(source_of - 1, limit - receiver)
    passed = jax.random.randint(jax.random.fold_in(rng, 1), (couples,), 0, 1 << 20) % (room + 1)
    sizes = sizes.at[1:1 + 2 * couples:2].set(source_of - passed).at[2:2 + 2 * couples:2].set(receiver + passed)
    return sizes[jax.random.permutation(jax.random.fold_in(rng, 2), count)]


def scatter_about(rng, extent, deviation, bound, cuts=(), held_as=jnp.bfloat16):
    level = level_of(rng, extent, cuts, -0.22, 0.18) if cuts else 1.0
    values = jax.random.normal(rng, extent, jnp.float32) * deviation * level
    return jnp.minimum(jnp.maximum(values, -bound), bound).astype(held_as)


def heavy_noise(stream_key, shape, scale, bound, shards, heavy, kind=jnp.bfloat16):
    array = scale * jax.random.normal(stream_key, shape, jnp.float32)
    if shards:
        array = array * level_of(stream_key, shape, shards, -0.22, 0.18)
    return jnp.clip(raised(array, jax.random.fold_in(stream_key, 3), *heavy), -bound, bound).astype(kind)


def setup_inputs(seed: int = 0) -> dict:
    arg_keys = jax.random.split(jax.random.key(seed), 13)
    return {
        "tokens": heavy_noise(arg_keys[0], (NSEQ, TOKS, D), 1.0, 6.0, ((0, 8), (1, 4)), (0, 2, 8, 2.0)),
        "qkv_weight": scatter_about(arg_keys[1], (D, 3 * D), D ** -0.5, 0.21875, ((0, 32),)),
        "out_weight": scatter_about(arg_keys[2], (D, D), (D // 16) ** -0.5, 0.875, ((0, 32),)),
        "up_weight": scatter_about(arg_keys[3], (D, FF), D ** -0.5, 0.21875, ((0, 32),)),
        "down_weight": scatter_about(arg_keys[4], (FF, D), FF ** -0.5, 0.109375, ((0, 32),)),
        "attn_gain": jnp.clip(1.0 + 0.1 * jax.random.normal(arg_keys[5], (D,), jnp.float32), 0.5, 1.5).astype(jnp.bfloat16),
        "attn_shift": scatter_about(arg_keys[6], (D,), 0.3, 1.5, ((0, 32),)),
        "ffn_gain": jnp.clip(1.0 + 0.1 * jax.random.normal(arg_keys[7], (D,), jnp.float32), 0.5, 1.5).astype(jnp.bfloat16),
        "ffn_shift": scatter_about(arg_keys[8], (D,), 0.3, 1.5, ((0, 32),)),
        "pass_embed": scatter_about(arg_keys[9], (R, D), 0.5, 3.0, ((1, 32),)),
        "segment_ids": jax.vmap(lambda own: jnp.searchsorted(jnp.cumsum(uneven(own, DOCS, TOKS, SEG_MOST, 0)), jnp.arange(TOKS), side="right"))(jax.random.split(arg_keys[10], NSEQ)).reshape((NSEQ, TOKS)).astype(jnp.int32),
        "cotangent": scatter_about(arg_keys[11], (NSEQ, TOKS * R, D), 1.0, 6.0, ((0, 8), (1, 4))),
    }


@jax.custom_vjp
def low(v):
    return lax.optimization_barrier(v.astype(jnp.bfloat16)).astype(jnp.float32)

@jax.custom_vjp
def low_back(v):
    return v

def low_keep(v):
    return (low(v), None)

def low_pass(kept, grad):
    return (grad,)

def back_keep(v):
    return (v, None)

def back_low(kept, grad):
    return (low(grad),)
low.defvjp(low_keep, low_pass)
low_back.defvjp(back_keep, back_low)

def layer_norm(entry, gain_row, shift_row):
    row_mean = lax.optimization_barrier(jnp.mean(entry, axis=-1, keepdims=True))
    centered = entry - row_mean
    variance = lax.optimization_barrier(jnp.mean(centered * centered, axis=-1, keepdims=True))
    return centered * lax.rsqrt(variance + 1e-05) * gain_row + shift_row

def matmul_high(form, first, second):
    return jnp.einsum(form, first, second, precision=lax.Precision.HIGHEST)

def forward_group(inputs, qkv_weight, out_weight, up_weight, down_weight, gain_first, shift_first, gain_second, shift_second, pass_rows, doc_ids):
    seq_count = inputs.shape[0]
    positions = jnp.arange(TOKS, dtype=jnp.int32)
    allowed = (doc_ids[:, :, None] == doc_ids[:, None, :]) & (positions[None, None, :] <= positions[None, :, None])
    current = inputs
    key_list = []
    value_list = []
    outputs = []
    for repeat in range(R):
        entry = current + pass_rows[repeat]
        normed = low(layer_norm(entry, gain_first, shift_first))
        projected = low(low_back(matmul_high('std,de->ste', normed, qkv_weight)))
        queries = projected[:, :, :D].reshape(seq_count, TOKS, H, HD)
        key_list.append(projected[:, :, D:2 * D].reshape(seq_count, TOKS, H, HD))
        value_list.append(projected[:, :, 2 * D:].reshape(seq_count, TOKS, H, HD))
        key_heads = jnp.concatenate(key_list, axis=1)
        value_heads = jnp.concatenate(value_list, axis=1)
        scores = low_back(matmul_high('sqhe,skhe->shqk', queries, key_heads) * 0.125)
        allowed_now = jnp.tile(allowed, (1, 1, repeat + 1))
        scores = jnp.where(allowed_now[:, None], scores, -1e+30)
        attn_probs = low(jax.nn.softmax(scores, axis=-1))
        attended = low(low_back(matmul_high('shqk,skhe->sqhe', attn_probs, value_heads)))
        attended = attended.reshape(seq_count, TOKS, D)
        middle = entry + low_back(matmul_high('std,de->ste', attended, out_weight))
        normed_mid = low(layer_norm(middle, gain_second, shift_second))
        hidden = low_back(matmul_high('std,de->ste', normed_mid, up_weight))
        activated = low(jax.nn.gelu(hidden, approximate=True))
        current = middle + low_back(matmul_high('std,de->ste', activated, down_weight))
        outputs.append(current)
    return jnp.stack(outputs, axis=2).reshape(seq_count, TOKS * R, D)

def reference(tokens, qkv_weight, out_weight, up_weight, down_weight, attn_gain, attn_shift, ffn_gain, ffn_shift, pass_embed, segment_ids, cotangent):
    params = tuple((member.astype(jnp.float32) for member in (qkv_weight, out_weight, up_weight, down_weight, attn_gain, attn_shift, ffn_gain, ffn_shift, pass_embed)))
    inputs = tokens.astype(jnp.float32).reshape(N_DP, SEQS, TOKS, D)
    doc_groups = segment_ids.reshape(N_DP, SEQS, TOKS)
    cot_groups = cotangent.astype(jnp.float32).reshape(N_DP, SEQS, TOKS * R, D)

    def group_step(totals, packed):
        group_in, group_ids, group_cot = packed

        def run_group(group_start, *weights):
            return forward_group(group_start, *weights, group_ids)
        result, pullback = jax.vjp(run_group, group_in, *params)
        grad_list = pullback(group_cot)
        new_totals = tuple((total + grad for total, grad in zip(totals, grad_list[1:])))
        return (new_totals, (result.astype(jnp.bfloat16), grad_list[0]))
    zero_totals = tuple((jnp.zeros_like(member) for member in params))
    totals, (activations, input_grads) = lax.scan(group_step, zero_totals, (inputs, doc_groups, cot_groups))
    return (activations.reshape(NSEQ, TOKS * R, D), input_grads.reshape(NSEQ, TOKS, D), totals[0], totals[1], totals[2], totals[3], totals[4], totals[5], totals[6], totals[7], totals[8])
```

```python
import jax
import jax.numpy as jnp
from jax import lax
from jax.experimental import pallas as pl
from jax.experimental.pallas import tpu as pltpu
from jax.sharding import PartitionSpec as P

H = 12
MESH = pl.DeviceIdType.MESH
F32 = jnp.float32
BF16 = jnp.bfloat16
VMEM_LIMIT = 62 * 2**20


def places():
    dp = lax.axis_index("dp")
    z = lax.axis_index("ctx")
    partner = dp + 1 - 2 * lax.rem(dp, 2)
    xdp = dp + 2 - 4 * lax.rem(dp // 2, 2)
    ydp = dp + 4 - 8 * (dp // 4)
    ddp = xdp + ydp - dp
    return dp, z, partner, xdp, ydp, ddp


def greet(dp, z, partner, xdp, ydp):
    bar = pltpu.get_barrier_semaphore()
    peers = [(partner, z), (xdp, z), (ydp, z)]
    peers += [(dp, lax.rem(z + step, 4)) for step in (1, 2, 3)]
    for peer in peers:
        pl.semaphore_signal(bar, inc=1, device_id=peer, device_id_type=MESH)
    pl.semaphore_wait(bar, len(peers))


def halves(width):
    first = (width // 256) * 128
    return pl.ds(0, first), pl.ds(first, width - first)


def gather_kernel(a_ref, b_ref, ao_ref, bo_ref, ssem, rsem, lsem):
    dp, z, partner, xdp, ydp, ddp = places()
    greet(dp, z, partner, xdp, ydp)
    pend = []
    pairs = ((a_ref, ao_ref), (b_ref, bo_ref))

    def view(ref, block, half):
        if half is None:
            return ref.at[block]
        return ref.at[block, :, halves(ref.shape[2])[half]]

    def send(block, to, slot, own=False, half=None):
        for t, (src, dst) in enumerate(pairs):
            target = view(dst, block, half)
            copy = pltpu.make_async_remote_copy(
                src_ref=src if own else target,
                dst_ref=target,
                send_sem=ssem.at[t, len(pend) // 2],
                recv_sem=rsem.at[t, slot],
                device_id=to,
                device_id_type=MESH,
            )
            copy.start()
            pend.append(copy)

    def wait(block, slot, half=None):
        for t, (_, dst) in enumerate(pairs):
            target = view(dst, block, half)
            pltpu.make_async_remote_copy(
                src_ref=target,
                dst_ref=target,
                send_sem=ssem.at[t, 0],
                recv_sem=rsem.at[t, slot],
                device_id=(partner, z),
                device_id_type=MESH,
            ).wait_recv()

    zs = [lax.rem(z + 4 - step, 4) for step in range(4)]
    me = dp * 4 + z
    send(me, (xdp, z), 3, own=True)
    send(me, (ydp, z), 7, own=True)
    for step in (1, 2, 3):
        send(me, (dp, lax.rem(z + step, 4)), step - 1, own=True)
    send(me, (partner, z), 19, own=True)
    local = [pltpu.make_async_copy(src, dst.at[me], lsem.at[t]) for t, (src, dst) in enumerate(pairs)]
    for copy in local:
        copy.start()

    def relay(j):
        bx, by = xdp * 4 + zs[j], ydp * 4 + zs[j]
        wait(bx, 3 + j)
        send(bx, (ydp, z), 11 + j, half=0)
        send(bx, (partner, z), 23 + j)
        wait(by, 7 + j)
        send(by, (xdp, z), 15 + j, half=1)
        send(by, (partner, z), 27 + j)

    for j in range(1, 4):
        block = dp * 4 + zs[j]
        wait(block, j - 1)
        send(block, (xdp, z), 3 + j)
        send(block, (ydp, z), 7 + j)
        send(block, (partner, z), 19 + j)
        relay(j - 1)
    relay(3)
    for j in range(4):
        block = ddp * 4 + zs[j]
        wait(block, 11 + j, 0)
        wait(block, 15 + j, 1)
        send(block, (partner, z), 31 + j)
    away = partner - dp
    for first, column in ((19, dp), (23, xdp), (27, ydp), (31, ddp)):
        for j in range(4):
            wait((column + away) * 4 + zs[j], first + j)
    for copy in local:
        copy.wait()
    for copy in pend:
        copy.wait_send()


def gather_blocks(a, b):
    count = lax.axis_size("dp") * lax.axis_size("ctx")
    return pl.pallas_call(
        gather_kernel,
        out_shape=(
            jax.ShapeDtypeStruct((count,) + a.shape, a.dtype),
            jax.ShapeDtypeStruct((count,) + b.shape, b.dtype),
        ),
        in_specs=[pl.BlockSpec(memory_space=pltpu.VMEM)] * 2,
        out_specs=[pl.BlockSpec(memory_space=pl.ANY)] * 2,
        scratch_shapes=[
            pltpu.SemaphoreType.DMA((2, 35)),
            pltpu.SemaphoreType.DMA((2, 35)),
            pltpu.SemaphoreType.DMA((2,)),
        ],
        compiler_params=pltpu.CompilerParams(collective_id=0, has_side_effects=True),
    )(a, b)


def reduce_kernel(
    a_hbm, b_hbm, ao_ref, bo_ref,
    la, lb, pa, pb, fxa, fxb, fya, fyb, hxa, hxb, hya, hyb, za, zb,
    lsem, ssem, rsem,
):
    dp, z, partner, xdp, ydp, ddp = places()
    greet(dp, z, partner, xdp, ydp)
    pend = []

    def send(sources, targets, to, slot):
        for t in (0, 1):
            copy = pltpu.make_async_remote_copy(
                src_ref=sources[t],
                dst_ref=targets[t],
                send_sem=ssem.at[t, len(pend) // 2],
                recv_sem=rsem.at[t, slot],
                device_id=to,
                device_id_type=MESH,
            )
            copy.start()
            pend.append(copy)

    def wait(targets, slot):
        for t in (0, 1):
            pltpu.make_async_remote_copy(
                src_ref=targets[t],
                dst_ref=targets[t],
                send_sem=ssem.at[t, 0],
                recv_sem=rsem.at[t, slot],
                device_id=(partner, z),
                device_id_type=MESH,
            ).wait_recv()

    zs = [lax.rem(z + 1 + j, 4) for j in range(4)]
    columns = (ddp, xdp, ydp, dp)
    order = [(0, 0), (0, 1), (1, 0), (2, 0), (0, 2), (1, 1), (2, 1), (3, 0)]
    order += [(0, 3), (1, 2), (2, 2), (3, 1), (1, 3), (2, 3), (3, 2), (3, 3)]
    loads = {}
    for c, j in order:
        s = c * 4 + j
        block = columns[c] * 4 + zs[j]
        other = block + (partner - dp) * 4
        send((a_hbm.at[other], b_hbm.at[other]), (pa.at[s], pb.at[s]), (partner, z), s)
        loads[s] = [
            pltpu.make_async_copy(src.at[block], dst.at[s], lsem.at[t, s])
            for t, (src, dst) in enumerate(((a_hbm, la), (b_hbm, lb)))
        ]
        for copy in loads[s]:
            copy.start()
    a_half = halves(a_hbm.shape[2])
    b_half = halves(b_hbm.shape[2])
    for c, j in order:
        s = c * 4 + j
        for copy in loads[s]:
            copy.wait()
        wait((pa.at[s], pb.at[s]), s)
        if c == 0:
            for mine, other in ((la, pa), (lb, pb)):
                mine[s] = (mine[s].astype(F32) + other[s].astype(F32)).astype(mine.dtype)
            send((la.at[s, :, a_half[0]], lb.at[s, :, b_half[0]]), (hxa.at[j], hxb.at[j]), (xdp, z), 16 + j)
            send((la.at[s, :, a_half[1]], lb.at[s, :, b_half[1]]), (hya.at[j], hyb.at[j]), (ydp, z), 20 + j)
        elif c < 3:
            got, slot, part = ((hya, hyb), 20, 1) if c == 1 else ((hxa, hxb), 16, 0)
            wait((got[0].at[j], got[1].at[j]), slot + j)
            for mine, other, extra, half in ((la, pa, got[0], a_half), (lb, pb, got[1], b_half)):
                plain, joined = half[1 - part], half[part]
                mine[s, :, plain] = (mine[s, :, plain].astype(F32) + other[s, :, plain].astype(F32)).astype(mine.dtype)
                mine[s, :, joined] = (
                    mine[s, :, joined].astype(F32) + other[s, :, joined].astype(F32) + extra[j].astype(F32)
                ).astype(mine.dtype)
            into, to, slot = ((fxa, fxb), xdp, 24) if c == 1 else ((fya, fyb), ydp, 28)
            send((la.at[s], lb.at[s]), (into[0].at[j], into[1].at[j]), (to, z), slot + j)
        else:
            wait((fxa.at[j], fxb.at[j]), 24 + j)
            wait((fya.at[j], fyb.at[j]), 28 + j)
            totals = [
                mine[s].astype(F32) + other[s].astype(F32) + first[j].astype(F32) + second[j].astype(F32)
                for mine, other, first, second in ((la, pa, fxa, fya), (lb, pb, fxb, fyb))
            ]
            if j < 3:
                la[s] = totals[0].astype(la.dtype)
                lb[s] = totals[1].astype(lb.dtype)
                send((la.at[s], lb.at[s]), (za.at[j], zb.at[j]), (dp, zs[j]), 32 + j)
            else:
                ao_ref[...] = totals[0]
                bo_ref[...] = totals[1]
    for j in range(3):
        wait((za.at[j], zb.at[j]), 32 + j)
        ao_ref[...] += za[j].astype(F32)
        bo_ref[...] += zb[j].astype(F32)
    for copy in pend:
        copy.wait_send()


def reduce_blocks(a, b):
    _, ra, ca = a.shape
    _, rb, cb = b.shape
    ha, hb = (ca // 256) * 128, (cb // 256) * 128

    def buffers(count, first, second):
        return [
            pltpu.VMEM((count, ra, ca if first is None else first), a.dtype),
            pltpu.VMEM((count, rb, cb if second is None else second), b.dtype),
        ]

    return pl.pallas_call(
        reduce_kernel,
        out_shape=(jax.ShapeDtypeStruct((ra, ca), F32), jax.ShapeDtypeStruct((rb, cb), F32)),
        in_specs=[pl.BlockSpec(memory_space=pl.ANY)] * 2,
        out_specs=[pl.BlockSpec(memory_space=pltpu.VMEM)] * 2,
        scratch_shapes=buffers(16, None, None)
        + buffers(16, None, None)
        + buffers(4, None, None)
        + buffers(4, None, None)
        + buffers(4, ha, hb)
        + buffers(4, ca - ha, cb - hb)
        + buffers(3, None, None)
        + [
            pltpu.SemaphoreType.DMA((2, 16)),
            pltpu.SemaphoreType.DMA((2, 35)),
            pltpu.SemaphoreType.DMA((2, 35)),
        ],
        compiler_params=pltpu.CompilerParams(
            collective_id=1, has_side_effects=True, vmem_limit_bytes=VMEM_LIMIT
        ),
    )(a, b)


def layer_norm(entry, gain_row, shift_row):
    row_mean = jnp.mean(entry, axis=-1, keepdims=True)
    centered = entry - row_mean
    variance = jnp.mean(centered * centered, axis=-1, keepdims=True)
    return centered * lax.rsqrt(variance + 1e-05) * gain_row + shift_row


def gelu_tanh(values):
    return jax.nn.gelu(values, approximate=True)


def project(features, matrix):
    return jnp.einsum("std,de->ste", features, matrix, preferred_element_type=jnp.float32)


def project_back(features, matrix):
    return jnp.einsum("ste,de->std", features, matrix, preferred_element_type=jnp.float32)


def outer_sum(feature_list, grad_list):
    features = jnp.concatenate(feature_list, axis=1)
    grads_in = jnp.concatenate(grad_list, axis=1)
    return jnp.einsum("std,ste->de", features, grads_in, preferred_element_type=jnp.float32)


def split_heads(tensor, head_count):
    return tensor.reshape(
        tensor.shape[0], tensor.shape[1], head_count, tensor.shape[2] // head_count
    )


def merge_heads(tensor):
    return tensor.reshape(tensor.shape[0], tensor.shape[1], tensor.shape[2] * tensor.shape[3])


def stored_keys(kv_store, pass_count, model_width, head_count):
    joined = jnp.concatenate(kv_store[:pass_count], axis=1)
    return (
        split_heads(joined[:, :, :model_width], head_count),
        split_heads(joined[:, :, model_width:], head_count),
    )


def score_block(queries, key_heads, allowed_now):
    scores = (
        jnp.einsum("sqhe,skhe->shqk", queries, key_heads, preferred_element_type=jnp.float32)
        * 0.125
    )
    return jnp.where(allowed_now[:, None], scores, -1e30)


def on_device(
    tokens,
    qkv_weight,
    out_weight,
    up_weight,
    down_weight,
    attn_gain,
    attn_shift,
    ffn_gain,
    ffn_shift,
    pass_embed,
    segment_ids,
    cotangent,
):
    seq_count, local_tok, model_width = tokens.shape
    repeats = pass_embed.shape[0]
    head_count = H
    full_tok = local_tok * lax.axis_size("ctx")
    all_ids = lax.all_gather(segment_ids, "ctx", axis=1, tiled=True)
    query_pos = lax.axis_index("ctx") * local_tok + jnp.arange(local_tok, dtype=jnp.int32)
    key_pos = jnp.arange(full_tok, dtype=jnp.int32)
    allowed = (segment_ids[:, :, None] == all_ids[:, None, :]) & (
        key_pos[None, None, :] <= query_pos[None, :, None]
    )
    current = tokens.astype(jnp.float32)
    log_totals = []
    kv_store = []
    pass_outputs = []
    normed_keep = []
    query_keep = []
    attended_keep = []
    normed_mid_keep = []
    activated_keep = []
    first_backs = []
    second_backs = []
    gelu_backs = []
    small_in = jnp.stack([attn_gain, attn_shift, ffn_gain, ffn_shift], axis=1)
    small_in = jnp.concatenate([small_in, pass_embed.T], axis=1)
    small_in = jnp.pad(small_in, ((0, 0), (0, 128 - small_in.shape[1])))
    rows_a = jnp.concatenate([qkv_weight, out_weight, up_weight, small_in], axis=1)
    if (lax.axis_size("dp"), lax.axis_size("ctx")) == (8, 4):
        all_a, all_b = gather_blocks(rows_a, down_weight)
    else:
        all_a = lax.all_gather(rows_a, ("dp", "ctx"), axis=0)
        all_b = lax.all_gather(down_weight, ("dp", "ctx"), axis=0)
    all_a = all_a.reshape(model_width, -1)
    down_full = all_b.reshape(-1, model_width)
    qkv_cols, ff_width = qkv_weight.shape[1], up_weight.shape[1]
    qkv_full = all_a[:, :qkv_cols]
    out_full = all_a[:, qkv_cols : qkv_cols + model_width]
    up_full = all_a[:, qkv_cols + model_width : qkv_cols + model_width + ff_width]
    small_rows = all_a[:, qkv_cols + model_width + ff_width :].T
    gain_first, shift_first, gain_second, shift_second = (small_rows[row] for row in range(4))
    embed_full = small_rows[4 : 4 + repeats]
    for repeat in range(repeats):
        entry = current + embed_full[repeat].astype(jnp.float32)
        normed, norm_first_back = jax.vjp(
            layer_norm, entry, gain_first.astype(jnp.float32), shift_first.astype(jnp.float32)
        )
        normed_lo = normed.astype(jnp.bfloat16)
        projected = project(normed_lo, qkv_full).astype(jnp.bfloat16)
        local_kv = projected[:, :, model_width:]
        kv_store.append(lax.all_gather(local_kv, "ctx", axis=1, tiled=True))
        key_heads, value_heads = stored_keys(kv_store, repeat + 1, model_width, head_count)
        queries = split_heads(projected[:, :, :model_width], head_count)
        allowed_now = jnp.tile(allowed, (1, 1, repeat + 1))
        scores = score_block(queries, key_heads, allowed_now)
        row_max = jnp.max(scores, axis=-1, keepdims=True)
        shifted = jnp.exp(scores - row_max)
        total_exp = jnp.sum(shifted, axis=-1, keepdims=True)
        log_totals.append(row_max + jnp.log(total_exp))
        probs_lo = (shifted / total_exp).astype(jnp.bfloat16)
        attended = merge_heads(
            jnp.einsum("shqk,skhe->sqhe", probs_lo, value_heads, preferred_element_type=jnp.float32)
        ).astype(jnp.bfloat16)
        middle = entry + project(attended, out_full)
        normed_mid, norm_second_back = jax.vjp(
            layer_norm, middle, gain_second.astype(jnp.float32), shift_second.astype(jnp.float32)
        )
        normed_mid_lo = normed_mid.astype(jnp.bfloat16)
        activated, gelu_back = jax.vjp(gelu_tanh, project(normed_mid_lo, up_full))
        activated_lo = activated.astype(jnp.bfloat16)
        current = middle + project(activated_lo, down_full)
        pass_outputs.append(current.astype(jnp.bfloat16))
        normed_keep.append(normed_lo)
        query_keep.append(queries)
        attended_keep.append(attended)
        normed_mid_keep.append(normed_mid_lo)
        activated_keep.append(activated_lo)
        first_backs.append(norm_first_back)
        second_backs.append(norm_second_back)
        gelu_backs.append(gelu_back)
    small_totals = [jnp.zeros((model_width,), jnp.float32) for slot in range(4)]
    key_grads = [
        jnp.zeros((seq_count, full_tok, 2 * model_width), jnp.float32) for earlier in range(repeats)
    ]
    branch_keep = [None] * repeats
    hidden_keep = [None] * repeats
    attn_out_keep = [None] * repeats
    proj_keep = [None] * repeats
    embed_rows = [None] * repeats
    carry = jnp.zeros((seq_count, local_tok, model_width), jnp.float32)
    cot_split = cotangent.reshape(seq_count, local_tok, repeats, model_width)
    for repeat in reversed(range(repeats)):
        grad_out = cot_split[:, :, repeat].astype(jnp.float32) + carry
        queries = query_keep[repeat]
        key_heads, value_heads = stored_keys(kv_store, repeat + 1, model_width, head_count)
        allowed_now = jnp.tile(allowed, (1, 1, repeat + 1))
        attn_probs = jnp.exp(score_block(queries, key_heads, allowed_now) - log_totals[repeat])
        probs_lo = attn_probs.astype(jnp.bfloat16)
        branch_grad = grad_out.astype(jnp.bfloat16)
        branch_keep[repeat] = branch_grad
        hidden_grad = gelu_backs[repeat](project_back(branch_grad, down_full))[0].astype(
            jnp.bfloat16
        )
        hidden_keep[repeat] = hidden_grad
        middle_grad, gain_second_grad, shift_second_grad = second_backs[repeat](
            project_back(hidden_grad, up_full)
        )
        small_totals[2] = small_totals[2] + gain_second_grad
        small_totals[3] = small_totals[3] + shift_second_grad
        middle_grad = middle_grad + grad_out
        attn_out_grad = middle_grad.astype(jnp.bfloat16)
        attn_out_keep[repeat] = attn_out_grad
        mixed_grad = split_heads(
            project_back(attn_out_grad, out_full).astype(jnp.bfloat16), head_count
        )
        prob_grad = jnp.einsum(
            "sqhe,skhe->shqk", mixed_grad, value_heads, preferred_element_type=jnp.float32
        )
        score_grad = (
            attn_probs * (prob_grad - jnp.sum(prob_grad * attn_probs, axis=-1, keepdims=True))
        ).astype(jnp.bfloat16)
        query_grad = (
            jnp.einsum("shqk,skhe->sqhe", score_grad, key_heads, preferred_element_type=jnp.float32)
            * 0.125
        )
        key_grad = (
            jnp.einsum("shqk,sqhe->skhe", score_grad, queries, preferred_element_type=jnp.float32)
            * 0.125
        )
        value_grad = jnp.einsum(
            "shqk,sqhe->skhe", probs_lo, mixed_grad, preferred_element_type=jnp.float32
        )
        joined_grad = jnp.concatenate([merge_heads(key_grad), merge_heads(value_grad)], axis=-1)
        for earlier in range(repeat + 1):
            key_grads[earlier] = (
                key_grads[earlier] + joined_grad[:, earlier * full_tok : (earlier + 1) * full_tok]
            )
        pass_grads = key_grads[repeat]
        own_grad = lax.psum_scatter(
            pass_grads.astype(jnp.bfloat16), "ctx", scatter_dimension=1, tiled=True
        ).astype(jnp.float32)
        proj_grad = jnp.concatenate([merge_heads(query_grad), own_grad], axis=-1).astype(
            jnp.bfloat16
        )
        proj_keep[repeat] = proj_grad
        entry_grad, gain_first_grad, shift_first_grad = first_backs[repeat](
            project_back(proj_grad, qkv_full)
        )
        small_totals[0] = small_totals[0] + gain_first_grad
        small_totals[1] = small_totals[1] + shift_first_grad
        carry = entry_grad + middle_grad
        embed_rows[repeat] = jnp.sum(carry, axis=(0, 1))
    qkv_total = outer_sum(normed_keep, proj_keep)
    out_total = outer_sum(attended_keep, attn_out_keep)
    up_total = outer_sum(normed_mid_keep, hidden_keep)
    down_total = outer_sum(activated_keep, branch_keep)
    embed_grad = jnp.stack(embed_rows, axis=0)
    small_total = jnp.concatenate([jnp.stack(small_totals, axis=0), embed_grad], axis=0).T
    small_total = jnp.pad(small_total, ((0, 0), (0, 128 - small_total.shape[1])))
    grad_a = jnp.concatenate(
        [qkv_total.astype(jnp.bfloat16), out_total.astype(jnp.bfloat16), up_total.astype(jnp.bfloat16), small_total.astype(jnp.bfloat16)], axis=1
    ).reshape(-1, *rows_a.shape)
    grad_b = down_total.astype(jnp.bfloat16).reshape(-1, *down_weight.shape)
    if (lax.axis_size("dp"), lax.axis_size("ctx")) == (8, 4):
        own_a, own_b = reduce_blocks(grad_a, grad_b)
    else:
        own_a = lax.psum_scatter(grad_a.astype(jnp.float32), ("dp", "ctx"), scatter_dimension=0)
        own_b = lax.psum_scatter(grad_b.astype(jnp.float32), ("dp", "ctx"), scatter_dimension=0)
    own_small = own_a[:, qkv_cols + model_width + ff_width :].T
    reduced = (
        own_a[:, :qkv_cols],
        own_a[:, qkv_cols : qkv_cols + model_width],
        own_a[:, qkv_cols + model_width : qkv_cols + model_width + ff_width],
        own_b,
        own_small[0],
        own_small[1],
        own_small[2],
        own_small[3],
        own_small[4 : 4 + repeats],
    )
    activations = jnp.stack(pass_outputs, axis=2).reshape(
        seq_count, local_tok * repeats, model_width
    )
    return (
        activations,
        carry,
        reduced[0],
        reduced[1],
        reduced[2],
        reduced[3],
        reduced[4],
        reduced[5],
        reduced[6],
        reduced[7],
        reduced[8],
    )


def solution(mesh):
    return jax.shard_map(
        on_device,
        mesh=mesh,
        in_specs=(
            P("dp", "ctx", None),
            P(("dp", "ctx"), None),
            P(("dp", "ctx"), None),
            P(("dp", "ctx"), None),
            P(("dp", "ctx"), None),
            P(("dp", "ctx")),
            P(("dp", "ctx")),
            P(("dp", "ctx")),
            P(("dp", "ctx")),
            P(None, ("dp", "ctx")),
            P("dp", "ctx"),
            P("dp", "ctx", None),
        ),
        out_specs=(
            P("dp", "ctx", None),
            P("dp", "ctx", None),
            P(("dp", "ctx"), None),
            P(("dp", "ctx"), None),
            P(("dp", "ctx"), None),
            P(("dp", "ctx"), None),
            P(("dp", "ctx")),
            P(("dp", "ctx")),
            P(("dp", "ctx")),
            P(("dp", "ctx")),
            P(None, ("dp", "ctx")),
        ),
        check_vma=False,
    )
```

```python
import jax
import jax.numpy as jnp
from jax import lax
from jax.experimental import pallas as pl
from jax.experimental.pallas import tpu as pltpu
from jax.sharding import PartitionSpec as P

H = 12
MESH = pl.DeviceIdType.MESH
F32 = jnp.float32
BF16 = jnp.bfloat16
VMEM_LIMIT = 62 * 2**20


def places():
    dp = lax.axis_index("dp")
    z = lax.axis_index("ctx")
    partner = dp + 1 - 2 * lax.rem(dp, 2)
    xdp = dp + 2 - 4 * lax.rem(dp // 2, 2)
    ydp = dp + 4 - 8 * (dp // 4)
    ddp = xdp + ydp - dp
    return dp, z, partner, xdp, ydp, ddp


def greet(dp, z, partner, xdp, ydp):
    bar = pltpu.get_barrier_semaphore()
    peers = [(partner, z), (xdp, z), (ydp, z)]
    peers += [(dp, lax.rem(z + step, 4)) for step in (1, 2, 3)]
    for peer in peers:
        pl.semaphore_signal(bar, inc=1, device_id=peer, device_id_type=MESH)
    pl.semaphore_wait(bar, len(peers))


def halves(width):
    first = (width // 256) * 128
    return pl.ds(0, first), pl.ds(first, width - first)


def gather_kernel(a_ref, b_ref, ao_ref, bo_ref, ssem, rsem, lsem):
    dp, z, partner, xdp, ydp, ddp = places()
    greet(dp, z, partner, xdp, ydp)
    pend = []
    pairs = ((a_ref, ao_ref), (b_ref, bo_ref))

    def view(ref, block, half):
        if half is None:
            return ref.at[block]
        return ref.at[block, :, halves(ref.shape[2])[half]]

    def send(block, to, slot, own=False, half=None):
        for t, (src, dst) in enumerate(pairs):
            target = view(dst, block, half)
            copy = pltpu.make_async_remote_copy(
                src_ref=src if own else target,
                dst_ref=target,
                send_sem=ssem.at[t, len(pend) // 2],
                recv_sem=rsem.at[t, slot],
                device_id=to,
                device_id_type=MESH,
            )
            copy.start()
            pend.append(copy)

    def wait(block, slot, half=None):
        for t, (_, dst) in enumerate(pairs):
            target = view(dst, block, half)
            pltpu.make_async_remote_copy(
                src_ref=target,
                dst_ref=target,
                send_sem=ssem.at[t, 0],
                recv_sem=rsem.at[t, slot],
                device_id=(partner, z),
                device_id_type=MESH,
            ).wait_recv()

    zs = [lax.rem(z + 4 - step, 4) for step in range(4)]
    me = dp * 4 + z
    send(me, (xdp, z), 3, own=True)
    send(me, (ydp, z), 7, own=True)
    for step in (1, 2, 3):
        send(me, (dp, lax.rem(z + step, 4)), step - 1, own=True)
    send(me, (partner, z), 19, own=True)
    local = [pltpu.make_async_copy(src, dst.at[me], lsem.at[t]) for t, (src, dst) in enumerate(pairs)]
    for copy in local:
        copy.start()

    def relay(j):
        bx, by = xdp * 4 + zs[j], ydp * 4 + zs[j]
        wait(bx, 3 + j)
        send(bx, (ydp, z), 11 + j, half=0)
        send(bx, (partner, z), 23 + j)
        wait(by, 7 + j)
        send(by, (xdp, z), 15 + j, half=1)
        send(by, (partner, z), 27 + j)

    for j in range(1, 4):
        block = dp * 4 + zs[j]
        wait(block, j - 1)
        send(block, (xdp, z), 3 + j)
        send(block, (ydp, z), 7 + j)
        send(block, (partner, z), 19 + j)
        relay(j - 1)
    relay(3)
    for j in range(4):
        block = ddp * 4 + zs[j]
        wait(block, 11 + j, 0)
        wait(block, 15 + j, 1)
        send(block, (partner, z), 31 + j)
    away = partner - dp
    for first, column in ((19, dp), (23, xdp), (27, ydp), (31, ddp)):
        for j in range(4):
            wait((column + away) * 4 + zs[j], first + j)
    for copy in local:
        copy.wait()
    for copy in pend:
        copy.wait_send()


def gather_blocks(a, b):
    count = lax.axis_size("dp") * lax.axis_size("ctx")
    return pl.pallas_call(
        gather_kernel,
        out_shape=(
            jax.ShapeDtypeStruct((count,) + a.shape, a.dtype),
            jax.ShapeDtypeStruct((count,) + b.shape, b.dtype),
        ),
        in_specs=[pl.BlockSpec(memory_space=pltpu.VMEM)] * 2,
        out_specs=[pl.BlockSpec(memory_space=pl.ANY)] * 2,
        scratch_shapes=[
            pltpu.SemaphoreType.DMA((2, 35)),
            pltpu.SemaphoreType.DMA((2, 35)),
            pltpu.SemaphoreType.DMA((2,)),
        ],
        compiler_params=pltpu.CompilerParams(collective_id=0, has_side_effects=True),
    )(a, b)


def reduce_kernel(
    a_hbm, b_hbm, ao_ref, bo_ref,
    la, lb, pa, pb, fxa, fxb, fya, fyb, hxa, hxb, hya, hyb, za, zb,
    lsem, ssem, rsem,
):
    dp, z, partner, xdp, ydp, ddp = places()
    greet(dp, z, partner, xdp, ydp)
    pend = []

    def send(sources, targets, to, slot):
        for t in (0, 1):
            copy = pltpu.make_async_remote_copy(
                src_ref=sources[t],
                dst_ref=targets[t],
                send_sem=ssem.at[t, len(pend) // 2],
                recv_sem=rsem.at[t, slot],
                device_id=to,
                device_id_type=MESH,
            )
            copy.start()
            pend.append(copy)

    def wait(targets, slot):
        for t in (0, 1):
            pltpu.make_async_remote_copy(
                src_ref=targets[t],
                dst_ref=targets[t],
                send_sem=ssem.at[t, 0],
                recv_sem=rsem.at[t, slot],
                device_id=(partner, z),
                device_id_type=MESH,
            ).wait_recv()

    zs = [lax.rem(z + 1 + j, 4) for j in range(4)]
    columns = (ddp, xdp, ydp, dp)
    order = [(0, 0), (0, 1), (1, 0), (2, 0), (0, 2), (1, 1), (2, 1), (3, 0)]
    order += [(0, 3), (1, 2), (2, 2), (3, 1), (1, 3), (2, 3), (3, 2), (3, 3)]
    loads = {}
    for c, j in order:
        s = c * 4 + j
        block = columns[c] * 4 + zs[j]
        other = block + (partner - dp) * 4
        send((a_hbm.at[other], b_hbm.at[other]), (pa.at[s], pb.at[s]), (partner, z), s)
        loads[s] = [
            pltpu.make_async_copy(src.at[block], dst.at[s], lsem.at[t, s])
            for t, (src, dst) in enumerate(((a_hbm, la), (b_hbm, lb)))
        ]
        for copy in loads[s]:
            copy.start()
    a_half = halves(a_hbm.shape[2])
    b_half = halves(b_hbm.shape[2])
    for c, j in order:
        s = c * 4 + j
        for copy in loads[s]:
            copy.wait()
        wait((pa.at[s], pb.at[s]), s)
        if c == 0:
            for mine, other in ((la, pa), (lb, pb)):
                mine[s] = (mine[s].astype(F32) + other[s].astype(F32)).astype(mine.dtype)
            send((la.at[s, :, a_half[0]], lb.at[s, :, b_half[0]]), (hxa.at[j], hxb.at[j]), (xdp, z), 16 + j)
            send((la.at[s, :, a_half[1]], lb.at[s, :, b_half[1]]), (hya.at[j], hyb.at[j]), (ydp, z), 20 + j)
        elif c < 3:
            got, slot, part = ((hya, hyb), 20, 1) if c == 1 else ((hxa, hxb), 16, 0)
            wait((got[0].at[j], got[1].at[j]), slot + j)
            for mine, other, extra, half in ((la, pa, got[0], a_half), (lb, pb, got[1], b_half)):
                plain, joined = half[1 - part], half[part]
                mine[s, :, plain] = (mine[s, :, plain].astype(F32) + other[s, :, plain].astype(F32)).astype(mine.dtype)
                mine[s, :, joined] = (
                    mine[s, :, joined].astype(F32) + other[s, :, joined].astype(F32) + extra[j].astype(F32)
                ).astype(mine.dtype)
            into, to, slot = ((fxa, fxb), xdp, 24) if c == 1 else ((fya, fyb), ydp, 28)
            send((la.at[s], lb.at[s]), (into[0].at[j], into[1].at[j]), (to, z), slot + j)
        else:
            wait((fxa.at[j], fxb.at[j]), 24 + j)
            wait((fya.at[j], fyb.at[j]), 28 + j)
            totals = [
                mine[s].astype(F32) + other[s].astype(F32) + first[j].astype(F32) + second[j].astype(F32)
                for mine, other, first, second in ((la, pa, fxa, fya), (lb, pb, fxb, fyb))
            ]
            if j < 3:
                la[s] = totals[0].astype(la.dtype)
                lb[s] = totals[1].astype(lb.dtype)
                send((la.at[s], lb.at[s]), (za.at[j], zb.at[j]), (dp, zs[j]), 32 + j)
            else:
                ao_ref[...] = totals[0]
                bo_ref[...] = totals[1]
    for j in range(3):
        wait((za.at[j], zb.at[j]), 32 + j)
        ao_ref[...] += za[j].astype(F32)
        bo_ref[...] += zb[j].astype(F32)
    for copy in pend:
        copy.wait_send()


def reduce_blocks(a, b):
    _, ra, ca = a.shape
    _, rb, cb = b.shape
    ha, hb = (ca // 256) * 128, (cb // 256) * 128

    def buffers(count, first, second):
        return [
            pltpu.VMEM((count, ra, ca if first is None else first), a.dtype),
            pltpu.VMEM((count, rb, cb if second is None else second), b.dtype),
        ]

    return pl.pallas_call(
        reduce_kernel,
        out_shape=(jax.ShapeDtypeStruct((ra, ca), F32), jax.ShapeDtypeStruct((rb, cb), F32)),
        in_specs=[pl.BlockSpec(memory_space=pl.ANY)] * 2,
        out_specs=[pl.BlockSpec(memory_space=pltpu.VMEM)] * 2,
        scratch_shapes=buffers(16, None, None)
        + buffers(16, None, None)
        + buffers(4, None, None)
        + buffers(4, None, None)
        + buffers(4, ha, hb)
        + buffers(4, ca - ha, cb - hb)
        + buffers(3, None, None)
        + [
            pltpu.SemaphoreType.DMA((2, 16)),
            pltpu.SemaphoreType.DMA((2, 35)),
            pltpu.SemaphoreType.DMA((2, 35)),
        ],
        compiler_params=pltpu.CompilerParams(
            collective_id=1, has_side_effects=True, vmem_limit_bytes=VMEM_LIMIT
        ),
    )(a, b)


def ring():
    dp = lax.axis_index("dp")
    z = lax.axis_index("ctx")
    size = lax.axis_size("ctx")
    return z, (dp, lax.rem(z + 1, size)), (dp, lax.rem(z + size - 1, size))


def mm(x, w):
    return jnp.dot(x, w, preferred_element_type=F32)


def mm_nt(x, w):
    return lax.dot_general(x, w, (((1,), (1,)), ((), ())), preferred_element_type=F32)


def mm_tn(x, w):
    return lax.dot_general(x, w, (((0,), (0,)), ((), ())), preferred_element_type=F32)


def row_mean(values):
    return jnp.mean(values, axis=-1, keepdims=True)


def norm_forward(entry):
    centered = entry - row_mean(entry)
    scale = lax.rsqrt(row_mean(centered * centered) + 1e-05)
    return centered * scale, scale


def norm_backward(grad, gain, unit, scale):
    e = grad * gain
    return (e - row_mean(e) - unit * row_mean(e * unit)) * scale


def split_pair(pair):
    lane = lax.broadcasted_iota(jnp.int32, pair.shape, 1)
    zero = jnp.zeros_like(pair)
    return jnp.concatenate([jnp.where(lane < 64, pair, zero), jnp.where(lane < 64, zero, pair)], axis=0)


def join_pair(both):
    half = both.shape[0] // 2
    lane = lax.broadcasted_iota(jnp.int32, (half, 128), 1)
    return jnp.where(lane < 64, both[:half], both[half:])


def block_kernel(
    a_hbm, b_hbm, tok_ref, cot_ref, ids_ref,
    act_ref, ig_ref, ga_hbm, gb_hbm,
    wa, wb, small, cur, mid, kv, dkv, ids_got, bias, bias_t,
    normed_s, unit1, scale1, q_s, att_s, unit2, scale2, nm_s, slope_s, actv_s, lse_s,
    branch_s, hg_s, aog_s, pg_s, qbd, dobd, delta_s, m_s, l_s, acc_s, sums,
    far_out, near_out, far_in, near_in, stage,
    wsem, isem, fsend, frecv, bsend, brecv, gsem,
):
    chunk, nxt, prv = ring()
    T = tok_ref.shape[0]
    D = tok_ref.shape[1]
    R = cot_ref.shape[0]
    FF = wb.shape[0]
    pairs = D // 128
    S = 3 * T
    q_cols, kv_cols = pl.ds(0, D), pl.ds(D, 2 * D)
    out_cols = pl.ds(3 * D, D)
    up0 = 4 * D
    small0 = up0 + FF

    barrier = pltpu.get_barrier_semaphore()
    for peer in (nxt, prv):
        pl.semaphore_signal(barrier, inc=1, device_id=peer, device_id_type=MESH)
    parts = (
        (a_hbm.at[:, pl.ds(small0, 128)], wa.at[:, pl.ds(small0, 128)]),
        (a_hbm.at[:, pl.ds(0, 3 * D)], wa.at[:, pl.ds(0, 3 * D)]),
        (a_hbm.at[:, out_cols], wa.at[:, out_cols]),
        (a_hbm.at[:, pl.ds(up0, FF)], wa.at[:, pl.ds(up0, FF)]),
        (b_hbm, wb),
    )
    fetch = [pltpu.make_async_copy(src, dst, wsem.at[n]) for n, (src, dst) in enumerate(parts)]
    for copy in fetch:
        copy.start()
    pl.semaphore_wait(barrier, 2)

    def remote(src, dst, send_sem, recv_sem, to):
        return pltpu.make_async_remote_copy(
            src_ref=src, dst_ref=dst, send_sem=send_sem, recv_sem=recv_sem, device_id=to, device_id_type=MESH
        )

    first_ids = remote(ids_ref.at[pl.ds(1, 2)], ids_got.at[pl.ds(0, 2)], isem.at[0], isem.at[1], nxt)
    first_ids.start()
    cur[...] = tok_ref[...].astype(F32)
    sums[...] = jnp.zeros_like(sums)
    fetch[0].wait()
    small[...] = jnp.transpose(wa[:, pl.ds(small0, 128)].astype(F32))

    @pl.loop(0, R * 3)
    def _(step):
        dkv[pl.ds(pl.multiple_of(step * T, T), T), :] = jnp.zeros((T, 2 * D), F32)

    first_ids.wait()
    second_ids = remote(ids_got.at[1], ids_got.at[2], isem.at[2], isem.at[3], nxt)
    second_ids.start()
    second_ids.wait()
    key_row = ids_ref[0, 0:1, :] + ids_got[0, 0:1, :] + ids_got[2, 0:1, :]
    own_row = ids_ref[0, 0:1, 0:128] + ids_ref[1, 0:1, 0:128]
    own_col = jnp.transpose(jnp.broadcast_to(own_row, (128, 128)))[:, 0:1]
    shape = (2 * T, 4 * T)
    key = lax.broadcasted_iota(jnp.int32, shape, 1)
    query = lax.broadcasted_iota(jnp.int32, shape, 0)
    query = jnp.where(query >= T, query - T, query)
    slot = key // T
    allowed = (jnp.broadcast_to(key_row, shape) == jnp.broadcast_to(own_col, shape)) & (slot < 3)
    allowed = allowed & (slot <= chunk) & ((slot > 0) | (key <= query))
    full_bias = jnp.where(allowed, 0.0, -1e30).astype(F32)
    bias[...] = full_bias
    bias_t[...] = jnp.transpose(full_bias)

    def small_row(index):
        return small[pl.ds(index, 1), :]

    def rows(r):
        return pl.ds(pl.multiple_of(r * T, T), T)

    def keys(r, first, count):
        return pl.ds(pl.multiple_of(r * S + first * T, T), count * T)

    def kv_copies(r):
        own, near, far = keys(r, 0, 1), keys(r, 1, 1), keys(r, 2, 1)
        return (
            remote(kv.at[own], kv.at[near], fsend.at[0, r], frecv.at[0, r], nxt),
            remote(kv.at[near], kv.at[far], fsend.at[1, r], frecv.at[1, r], nxt),
        )

    def attend(row_slice, lanes):
        for p in range(pairs):
            cols = pl.ds(p * 128, 128)
            state = pl.ds(p * 128, 128)
            values = pl.ds(D + p * 128, 128)
            scores = mm_nt(qbd[state, :], kv[row_slice, cols]) + bias[:, lanes]
            old = m_s[state, :]
            new = jnp.maximum(old, jnp.max(scores, axis=-1, keepdims=True))
            weight = jnp.exp(scores - new[:, 0:1])
            shrink = jnp.exp(old - new)
            m_s[state, :] = new
            l_s[state, :] = l_s[state, :] * shrink + jnp.sum(weight, axis=-1, keepdims=True)
            acc_s[state, :] = acc_s[state, :] * shrink + mm(weight.astype(BF16), kv[row_slice, values])

    def forward(r, carry):
        mine = rows(r)
        first, second = kv_copies(r)
        entry = cur[...] + small_row(4 + r)
        unit, scale = norm_forward(entry)
        unit1[mine, :] = unit
        scale1[mine, :] = jnp.broadcast_to(scale, (T, 128))
        normed = (unit * small_row(0) + small_row(1)).astype(BF16)
        normed_s[mine, :] = normed

        @pl.when(r == 0)
        def _():
            fetch[1].wait()

        kv[keys(r, 0, 1), :] = mm(normed, wa[:, kv_cols]).astype(BF16)
        first.start()
        queries = mm(normed, wa[:, q_cols]).astype(BF16) * jnp.asarray(0.125, BF16)
        q_s[mine, :] = queries
        for p in range(pairs):
            qbd[pl.ds(p * 128, 128), :] = split_pair(queries[:, p * 128 : p * 128 + 128])
        m_s[...] = jnp.full_like(m_s, -1e30)
        l_s[...] = jnp.zeros_like(l_s)
        acc_s[...] = jnp.zeros_like(acc_s)
        lax.fori_loop(0, r, lambda e, c: (attend(keys(e, 0, 3), pl.ds(0, S)), c)[1], 0)
        attend(keys(r, 0, 1), pl.ds(0, T))
        first.wait_recv()
        second.start()
        attend(keys(r, 1, 1), pl.ds(T, T))
        second.wait_recv()
        attend(keys(r, 2, 1), pl.ds(2 * T, T))
        for p in range(pairs):
            state = pl.ds(p * 128, 128)
            total = l_s[state, :]
            att_s[mine, pl.ds(p * 128, 128)] = join_pair(acc_s[state, :] / total).astype(BF16)
            lse_s[pl.ds(pl.multiple_of(r * 8, 8), 8), pl.ds(p * 128, 128)] = jnp.transpose(
                m_s[state, :] + jnp.log(total)
            )[0:8, :]

        @pl.when(r == 0)
        def _():
            fetch[2].wait()

        middle = entry + mm(att_s[mine, :], wa[:, out_cols])
        unit, scale = norm_forward(middle)
        unit2[mine, :] = unit
        scale2[mine, :] = jnp.broadcast_to(scale, (T, 128))
        normed = (unit * small_row(2) + small_row(3)).astype(BF16)
        nm_s[mine, :] = normed

        @pl.when(r == 0)
        def _():
            fetch[3].wait()
            fetch[4].wait()

        total = middle
        for j in range(FF // D):
            hidden = mm(normed, wa[:, pl.ds(up0 + j * D, D)])
            square = hidden * hidden
            root = 0.7978845608028654
            t = jnp.tanh(root * hidden * (1.0 + 0.044715 * square))
            slope_s[mine, pl.ds(j * D, D)] = 0.5 * (1.0 + t) + 0.5 * root * hidden * (1.0 - t * t) * (
                1.0 + 3 * 0.044715 * square
            )
            activated = (0.5 * hidden * (1.0 + t)).astype(BF16)
            actv_s[mine, pl.ds(j * D, D)] = activated
            total = total + mm(activated, wb[pl.ds(j * D, D), :])
        cur[...] = total
        act_ref[r] = total.astype(BF16)
        first.wait_send()
        second.wait_send()
        return carry

    lax.fori_loop(0, R, forward, 0)
    cur[...] = jnp.zeros_like(cur)

    def grad_block(e):
        block = keys(e, 0, 3)
        for p in range(pairs):
            cols = pl.ds(p * 128, 128)
            state = pl.ds(p * 128, 128)
            values = pl.ds(D + p * 128, 128)
            k_pair, v_pair = kv[block, cols], kv[block, values]
            q_pair, o_pair = qbd[state, :], dobd[state, :]
            scores = mm_nt(k_pair, q_pair) + bias_t[0:S, :]
            probs = jnp.exp(scores - delta_s[0:1, cols])
            grad = probs * (mm_nt(v_pair, o_pair) - delta_s[8:9, cols])
            low = grad.astype(BF16)
            dkv[block, cols] += mm(low, q_pair)
            dkv[block, values] += mm(probs.astype(BF16), o_pair)
            acc_s[state, :] += mm_tn(low, k_pair)

    def backward(i, carry):
        r = R - 1 - i
        mine = rows(r)
        grad_out = cot_ref[r].astype(F32) + cur[...]
        branch = grad_out.astype(BF16)
        branch_s[mine, :] = branch
        e = jnp.zeros((T, D), F32)
        for j in range(FF // D):
            part = pl.ds(j * D, D)
            low = (mm_nt(branch, wb[part, :]) * slope_s[mine, part]).astype(BF16)
            hg_s[mine, part] = low
            e = e + mm_nt(low, wa[:, pl.ds(up0 + j * D, D)])
        unit = unit2[mine, :]
        sums[2:3, :] += jnp.sum(e * unit, axis=0, keepdims=True)
        sums[3:4, :] += jnp.sum(e, axis=0, keepdims=True)
        middle_grad = grad_out + norm_backward(e, small_row(2), unit, scale2[mine, 0:1])
        mid[...] = middle_grad
        low = middle_grad.astype(BF16)
        aog_s[mine, :] = low
        mixed = mm_nt(low, wa[:, out_cols]).astype(BF16)
        queries = q_s[mine, :]
        attended = att_s[mine, :]
        for p in range(pairs):
            state = pl.ds(p * 128, 128)
            lo, hi = p * 128, p * 128 + 128
            qbd[state, :] = split_pair(queries[:, lo:hi])
            o_pair = split_pair(mixed[:, lo:hi])
            dobd[state, :] = o_pair
            twice = jnp.concatenate([attended[:, lo:hi], attended[:, lo:hi]], axis=0)
            product = jnp.transpose(o_pair.astype(F32) * twice.astype(F32))
            delta_s[8:16, lo:hi] = jnp.broadcast_to(jnp.sum(product, axis=0, keepdims=True), (8, 128))
        delta_s[0:8, :] = lse_s[pl.ds(pl.multiple_of(r * 8, 8), 8), :]
        acc_s[...] = jnp.zeros_like(acc_s)
        grad_block(r)
        far_out[r] = dkv[keys(r, 2, 1), :].astype(BF16)
        far = remote(far_out.at[r], far_in.at[r], bsend.at[0, r], brecv.at[0, r], prv)
        far.start()
        lax.fori_loop(0, r, lambda e, c: (grad_block(e), c)[1], 0)
        far.wait_recv()
        near_out[r] = (dkv[keys(r, 1, 1), :] + far_in[r].astype(F32)).astype(BF16)
        near = remote(near_out.at[r], near_in.at[r], bsend.at[1, r], brecv.at[1, r], prv)
        near.start()
        for p in range(pairs):
            pg_s[mine, pl.ds(p * 128, 128)] = (0.125 * join_pair(acc_s[pl.ds(p * 128, 128), :])).astype(BF16)
        e = mm_nt(pg_s[mine, q_cols], wa[:, q_cols])
        near.wait_recv()
        low = (dkv[keys(r, 0, 1), :] + near_in[r].astype(F32)).astype(BF16)
        pg_s[mine, kv_cols] = low
        e = e + mm_nt(low, wa[:, kv_cols])
        unit = unit1[mine, :]
        sums[0:1, :] += jnp.sum(e * unit, axis=0, keepdims=True)
        sums[1:2, :] += jnp.sum(e, axis=0, keepdims=True)
        entry_grad = mid[...] + norm_backward(e, small_row(0), unit, scale1[mine, 0:1])
        cur[...] = entry_grad
        sums[pl.ds(4 + r, 1), :] = jnp.sum(entry_grad, axis=0, keepdims=True)
        far.wait_send()
        near.wait_send()
        return carry

    lax.fori_loop(0, R, backward, 0)
    ig_ref[...] = cur[...]

    wa[:, pl.ds(small0, 128)] = jnp.transpose(sums[...]).astype(BF16)
    tail = pltpu.make_async_copy(wa.at[:, pl.ds(small0, 128)], ga_hbm.at[:, pl.ds(small0, 128)], wsem.at[0])
    tail.start()

    def piece(n, features, grads, target):
        hold = n % 2 if isinstance(n, int) else lax.rem(n, 2)
        copy = pltpu.make_async_copy(stage.at[hold], target, gsem.at[hold])
        if not (isinstance(n, int) and n < 2):
            @pl.when(n >= 2)
            def _():
                copy.wait()

        stage[hold] = mm_tn(features, grads).astype(BF16)
        copy.start()

    def wide(n0, count, feature_ref, grad_ref, col0):
        def body(j, c):
            part = pl.ds(pl.multiple_of(j * D, D), D)
            piece(n0 + j, feature_ref[...], grad_ref[:, part], ga_hbm.at[:, pl.ds(pl.multiple_of(col0 + j * D, D), D)])
            return c

        lax.fori_loop(0, count, body, 0)

    wide(0, 3, normed_s, pg_s, 0)
    wide(3, 1, att_s, aog_s, 3 * D)
    wide(4, FF // D, nm_s, hg_s, up0)

    def tall(j, c):
        part = pl.ds(pl.multiple_of(j * D, D), D)
        piece(4 + FF // D + j, actv_s[:, part], branch_s[...], gb_hbm.at[part, :])
        return c

    lax.fori_loop(0, FF // D, tall, 0)
    for hold in (0, 1):
        pltpu.make_async_copy(stage.at[hold], gb_hbm.at[pl.ds(0, D), :], gsem.at[hold]).wait()
    tail.wait()


def run_block(all_a, all_b, tokens, cot, ids):
    T, D = tokens.shape
    R = cot.shape[0]
    FF = all_b.shape[0]
    rows = R * T
    V = pltpu.VMEM
    DMA = pltpu.SemaphoreType.DMA
    return pl.pallas_call(
        block_kernel,
        out_shape=(
            jax.ShapeDtypeStruct((R, T, D), BF16),
            jax.ShapeDtypeStruct((T, D), F32),
            jax.ShapeDtypeStruct(all_a.shape, BF16),
            jax.ShapeDtypeStruct(all_b.shape, BF16),
        ),
        in_specs=[pl.BlockSpec(memory_space=pl.ANY)] * 2 + [pl.BlockSpec(memory_space=pltpu.VMEM)] * 3,
        out_specs=[pl.BlockSpec(memory_space=pltpu.VMEM)] * 2 + [pl.BlockSpec(memory_space=pl.ANY)] * 2,
        scratch_shapes=[
            V(all_a.shape, BF16), V(all_b.shape, BF16), V((128, D), F32), V((T, D), F32), V((T, D), F32),
            V((3 * rows, 2 * D), BF16), V((3 * rows, 2 * D), F32), V((3, 8, 256), F32),
            V((128, 256), F32), V((256, 128), F32),
            V((rows, D), BF16), V((rows, D), F32), V((rows, 128), F32), V((rows, D), BF16), V((rows, D), BF16),
            V((rows, D), F32), V((rows, 128), F32), V((rows, D), BF16), V((rows, FF), F32), V((rows, FF), BF16),
            V((8 * R, D), F32),
            V((rows, D), BF16), V((rows, FF), BF16), V((rows, D), BF16), V((rows, 3 * D), BF16),
            V((D, 128), BF16), V((D, 128), BF16), V((16, D), F32), V((D, 128), F32), V((D, 128), F32), V((D, 128), F32),
            V((128, D), F32),
            V((R, T, 2 * D), BF16), V((R, T, 2 * D), BF16), V((R, T, 2 * D), BF16), V((R, T, 2 * D), BF16),
            V((2, D, D), BF16),
            DMA((5,)), DMA((4,)), DMA((2, R)), DMA((2, R)), DMA((2, R)), DMA((2, R)), DMA((2,)),
        ],
        compiler_params=pltpu.CompilerParams(
            collective_id=2, has_side_effects=True, vmem_limit_bytes=VMEM_LIMIT
        ),
    )(all_a, all_b, tokens, cot, ids)


def on_device(
    tokens,
    qkv_weight,
    out_weight,
    up_weight,
    down_weight,
    attn_gain,
    attn_shift,
    ffn_gain,
    ffn_shift,
    pass_embed,
    segment_ids,
    cotangent,
):
    _, local_tok, model_width = tokens.shape
    repeats = pass_embed.shape[0]
    qkv_cols, ff_width = qkv_weight.shape[1], up_weight.shape[1]
    small_in = jnp.stack([attn_gain, attn_shift, ffn_gain, ffn_shift], axis=1)
    small_in = jnp.concatenate([small_in, pass_embed.T], axis=1)
    small_in = jnp.pad(small_in, ((0, 0), (0, 128 - small_in.shape[1])))
    rows_a = jnp.concatenate([qkv_weight, out_weight, up_weight, small_in], axis=1)
    block_of_slice = (lax.axis_size("dp"), lax.axis_size("ctx")) == (8, 4)
    if block_of_slice:
        all_a, all_b = gather_blocks(rows_a, down_weight)
    else:
        all_a = lax.all_gather(rows_a, ("dp", "ctx"), axis=0)
        all_b = lax.all_gather(down_weight, ("dp", "ctx"), axis=0)
    all_a = all_a.reshape(model_width, -1)
    all_b = all_b.reshape(-1, model_width)
    own_ids = segment_ids.astype(F32)
    ids = jnp.stack([jnp.pad(own_ids, ((0, 0), (s * local_tok, (3 - s) * local_tok))) for s in range(3)])
    ids = jnp.broadcast_to(ids, (3, 8, 4 * local_tok))
    cot = cotangent.reshape(local_tok, repeats, model_width).transpose(1, 0, 2)
    outputs, input_grad, grad_a, grad_b = run_block(all_a, all_b, tokens[0], cot, ids)
    grad_a = grad_a.reshape(-1, *rows_a.shape)
    grad_b = grad_b.reshape(-1, *down_weight.shape)
    if block_of_slice:
        own_a, own_b = reduce_blocks(grad_a, grad_b)
    else:
        own_a = lax.psum_scatter(grad_a.astype(F32), ("dp", "ctx"), scatter_dimension=0)
        own_b = lax.psum_scatter(grad_b.astype(F32), ("dp", "ctx"), scatter_dimension=0)
    own_small = own_a[:, qkv_cols + model_width + ff_width :].T
    activations = outputs.transpose(1, 0, 2).reshape(1, local_tok * repeats, model_width)
    return (
        activations,
        input_grad[None],
        own_a[:, :qkv_cols],
        own_a[:, qkv_cols : qkv_cols + model_width],
        own_a[:, qkv_cols + model_width : qkv_cols + model_width + ff_width],
        own_b,
        own_small[0],
        own_small[1],
        own_small[2],
        own_small[3],
        own_small[4 : 4 + repeats],
    )


def solution(mesh):
    return jax.shard_map(
        on_device,
        mesh=mesh,
        in_specs=(
            P("dp", "ctx", None),
            P(("dp", "ctx"), None),
            P(("dp", "ctx"), None),
            P(("dp", "ctx"), None),
            P(("dp", "ctx"), None),
            P(("dp", "ctx")),
            P(("dp", "ctx")),
            P(("dp", "ctx")),
            P(("dp", "ctx")),
            P(None, ("dp", "ctx")),
            P("dp", "ctx"),
            P("dp", "ctx", None),
        ),
        out_specs=(
            P("dp", "ctx", None),
            P("dp", "ctx", None),
            P(("dp", "ctx"), None),
            P(("dp", "ctx"), None),
            P(("dp", "ctx"), None),
            P(("dp", "ctx"), None),
            P(("dp", "ctx")),
            P(("dp", "ctx")),
            P(("dp", "ctx")),
            P(("dp", "ctx")),
            P(None, ("dp", "ctx")),
        ),
        check_vma=False,
    )
```

```python
import jax
import jax.numpy as jnp
from jax import lax
from jax.experimental import pallas as pl
from jax.experimental.pallas import tpu as pltpu
from jax.sharding import PartitionSpec as P

H = 12
MESH = pl.DeviceIdType.MESH
F32 = jnp.float32
BF16 = jnp.bfloat16
VMEM_LIMIT = 62 * 2**20


def places():
    dp = lax.axis_index("dp")
    z = lax.axis_index("ctx")
    partner = dp + 1 - 2 * lax.rem(dp, 2)
    xdp = dp + 2 - 4 * lax.rem(dp // 2, 2)
    ydp = dp + 4 - 8 * (dp // 4)
    ddp = xdp + ydp - dp
    return dp, z, partner, xdp, ydp, ddp


def greet(dp, z, partner, xdp, ydp):
    bar = pltpu.get_barrier_semaphore()
    peers = [(partner, z), (xdp, z), (ydp, z)]
    peers += [(dp, lax.rem(z + step, 4)) for step in (1, 2, 3)]
    for peer in peers:
        pl.semaphore_signal(bar, inc=1, device_id=peer, device_id_type=MESH)
    pl.semaphore_wait(bar, len(peers))


def halves(width):
    first = (width // 256) * 128
    return pl.ds(0, first), pl.ds(first, width - first)


def gather_kernel(a_ref, b_ref, ao_ref, bo_ref, ssem, rsem, lsem):
    dp, z, partner, xdp, ydp, ddp = places()
    greet(dp, z, partner, xdp, ydp)
    pend = []
    pairs = ((a_ref, ao_ref), (b_ref, bo_ref))

    def view(ref, block, half):
        if half is None:
            return ref.at[block]
        return ref.at[block, :, halves(ref.shape[2])[half]]

    def send(block, to, slot, own=False, half=None):
        for t, (src, dst) in enumerate(pairs):
            target = view(dst, block, half)
            copy = pltpu.make_async_remote_copy(
                src_ref=src if own else target,
                dst_ref=target,
                send_sem=ssem.at[t, len(pend) // 2],
                recv_sem=rsem.at[t, slot],
                device_id=to,
                device_id_type=MESH,
            )
            copy.start()
            pend.append(copy)

    def wait(block, slot, half=None):
        for t, (_, dst) in enumerate(pairs):
            target = view(dst, block, half)
            pltpu.make_async_remote_copy(
                src_ref=target,
                dst_ref=target,
                send_sem=ssem.at[t, 0],
                recv_sem=rsem.at[t, slot],
                device_id=(partner, z),
                device_id_type=MESH,
            ).wait_recv()

    zs = [lax.rem(z + 4 - step, 4) for step in range(4)]
    me = dp * 4 + z
    send(me, (xdp, z), 3, own=True)
    send(me, (ydp, z), 7, own=True)
    for step in (1, 2, 3):
        send(me, (dp, lax.rem(z + step, 4)), step - 1, own=True)
    send(me, (partner, z), 19, own=True)
    local = [pltpu.make_async_copy(src, dst.at[me], lsem.at[t]) for t, (src, dst) in enumerate(pairs)]
    for copy in local:
        copy.start()

    def relay(j):
        bx, by = xdp * 4 + zs[j], ydp * 4 + zs[j]
        wait(bx, 3 + j)
        send(bx, (ydp, z), 11 + j, half=0)
        send(bx, (partner, z), 23 + j)
        wait(by, 7 + j)
        send(by, (xdp, z), 15 + j, half=1)
        send(by, (partner, z), 27 + j)

    for j in range(1, 4):
        block = dp * 4 + zs[j]
        wait(block, j - 1)
        send(block, (xdp, z), 3 + j)
        send(block, (ydp, z), 7 + j)
        send(block, (partner, z), 19 + j)
        relay(j - 1)
    relay(3)
    for j in range(4):
        block = ddp * 4 + zs[j]
        wait(block, 11 + j, 0)
        wait(block, 15 + j, 1)
        send(block, (partner, z), 31 + j)
    away = partner - dp
    for first, column in ((19, dp), (23, xdp), (27, ydp), (31, ddp)):
        for j in range(4):
            wait((column + away) * 4 + zs[j], first + j)
    for copy in local:
        copy.wait()
    for copy in pend:
        copy.wait_send()


def gather_blocks(a, b):
    count = lax.axis_size("dp") * lax.axis_size("ctx")
    return pl.pallas_call(
        gather_kernel,
        out_shape=(
            jax.ShapeDtypeStruct((count,) + a.shape, a.dtype),
            jax.ShapeDtypeStruct((count,) + b.shape, b.dtype),
        ),
        in_specs=[pl.BlockSpec(memory_space=pltpu.VMEM)] * 2,
        out_specs=[pl.BlockSpec(memory_space=pl.ANY)] * 2,
        scratch_shapes=[
            pltpu.SemaphoreType.DMA((2, 35)),
            pltpu.SemaphoreType.DMA((2, 35)),
            pltpu.SemaphoreType.DMA((2,)),
        ],
        compiler_params=pltpu.CompilerParams(collective_id=0, has_side_effects=True),
    )(a, b)


def reduce_kernel(
    a_hbm, b_hbm, ao_ref, bo_ref,
    la, lb, pa, pb, fxa, fxb, fya, fyb, hxa, hxb, hya, hyb, za, zb,
    lsem, ssem, rsem,
):
    dp, z, partner, xdp, ydp, ddp = places()
    greet(dp, z, partner, xdp, ydp)
    pend = []

    def send(sources, targets, to, slot):
        for t in (0, 1):
            copy = pltpu.make_async_remote_copy(
                src_ref=sources[t],
                dst_ref=targets[t],
                send_sem=ssem.at[t, len(pend) // 2],
                recv_sem=rsem.at[t, slot],
                device_id=to,
                device_id_type=MESH,
            )
            copy.start()
            pend.append(copy)

    def wait(targets, slot):
        for t in (0, 1):
            pltpu.make_async_remote_copy(
                src_ref=targets[t],
                dst_ref=targets[t],
                send_sem=ssem.at[t, 0],
                recv_sem=rsem.at[t, slot],
                device_id=(partner, z),
                device_id_type=MESH,
            ).wait_recv()

    zs = [lax.rem(z + 1 + j, 4) for j in range(4)]
    columns = (ddp, xdp, ydp, dp)
    order = [(0, 0), (0, 1), (1, 0), (2, 0), (0, 2), (1, 1), (2, 1), (3, 0)]
    order += [(0, 3), (1, 2), (2, 2), (3, 1), (1, 3), (2, 3), (3, 2), (3, 3)]
    loads = {}
    for c, j in order:
        s = c * 4 + j
        block = columns[c] * 4 + zs[j]
        other = block + (partner - dp) * 4
        send((a_hbm.at[other], b_hbm.at[other]), (pa.at[s], pb.at[s]), (partner, z), s)
        loads[s] = [
            pltpu.make_async_copy(src.at[block], dst.at[s], lsem.at[t, s])
            for t, (src, dst) in enumerate(((a_hbm, la), (b_hbm, lb)))
        ]
        for copy in loads[s]:
            copy.start()
    a_half = halves(a_hbm.shape[2])
    b_half = halves(b_hbm.shape[2])
    for c, j in order:
        s = c * 4 + j
        for copy in loads[s]:
            copy.wait()
        wait((pa.at[s], pb.at[s]), s)
        if c == 0:
            for mine, other in ((la, pa), (lb, pb)):
                mine[s] = (mine[s].astype(F32) + other[s].astype(F32)).astype(mine.dtype)
            send((la.at[s, :, a_half[0]], lb.at[s, :, b_half[0]]), (hxa.at[j], hxb.at[j]), (xdp, z), 16 + j)
            send((la.at[s, :, a_half[1]], lb.at[s, :, b_half[1]]), (hya.at[j], hyb.at[j]), (ydp, z), 20 + j)
        elif c < 3:
            got, slot, part = ((hya, hyb), 20, 1) if c == 1 else ((hxa, hxb), 16, 0)
            wait((got[0].at[j], got[1].at[j]), slot + j)
            for mine, other, extra, half in ((la, pa, got[0], a_half), (lb, pb, got[1], b_half)):
                plain, joined = half[1 - part], half[part]
                mine[s, :, plain] = (mine[s, :, plain].astype(F32) + other[s, :, plain].astype(F32)).astype(mine.dtype)
                mine[s, :, joined] = (
                    mine[s, :, joined].astype(F32) + other[s, :, joined].astype(F32) + extra[j].astype(F32)
                ).astype(mine.dtype)
            into, to, slot = ((fxa, fxb), xdp, 24) if c == 1 else ((fya, fyb), ydp, 28)
            send((la.at[s], lb.at[s]), (into[0].at[j], into[1].at[j]), (to, z), slot + j)
        else:
            wait((fxa.at[j], fxb.at[j]), 24 + j)
            wait((fya.at[j], fyb.at[j]), 28 + j)
            totals = [
                mine[s].astype(F32) + other[s].astype(F32) + first[j].astype(F32) + second[j].astype(F32)
                for mine, other, first, second in ((la, pa, fxa, fya), (lb, pb, fxb, fyb))
            ]
            if j < 3:
                la[s] = totals[0].astype(la.dtype)
                lb[s] = totals[1].astype(lb.dtype)
                send((la.at[s], lb.at[s]), (za.at[j], zb.at[j]), (dp, zs[j]), 32 + j)
            else:
                ao_ref[...] = totals[0]
                bo_ref[...] = totals[1]
    for j in range(3):
        wait((za.at[j], zb.at[j]), 32 + j)
        ao_ref[...] += za[j].astype(F32)
        bo_ref[...] += zb[j].astype(F32)
    for copy in pend:
        copy.wait_send()


def reduce_blocks(a, b):
    _, ra, ca = a.shape
    _, rb, cb = b.shape
    ha, hb = (ca // 256) * 128, (cb // 256) * 128

    def buffers(count, first, second):
        return [
            pltpu.VMEM((count, ra, ca if first is None else first), a.dtype),
            pltpu.VMEM((count, rb, cb if second is None else second), b.dtype),
        ]

    return pl.pallas_call(
        reduce_kernel,
        out_shape=(jax.ShapeDtypeStruct((ra, ca), F32), jax.ShapeDtypeStruct((rb, cb), F32)),
        in_specs=[pl.BlockSpec(memory_space=pl.ANY)] * 2,
        out_specs=[pl.BlockSpec(memory_space=pltpu.VMEM)] * 2,
        scratch_shapes=buffers(16, None, None)
        + buffers(16, None, None)
        + buffers(4, None, None)
        + buffers(4, None, None)
        + buffers(4, ha, hb)
        + buffers(4, ca - ha, cb - hb)
        + buffers(3, None, None)
        + [
            pltpu.SemaphoreType.DMA((2, 16)),
            pltpu.SemaphoreType.DMA((2, 35)),
            pltpu.SemaphoreType.DMA((2, 35)),
        ],
        compiler_params=pltpu.CompilerParams(
            collective_id=1, has_side_effects=True, vmem_limit_bytes=VMEM_LIMIT
        ),
    )(a, b)


def ring():
    dp = lax.axis_index("dp")
    z = lax.axis_index("ctx")
    core = lax.rem(dp, 2)
    odd = lax.rem(z, 2)
    other = dp + 1 - 2 * core
    across = 1 - 2 * odd
    return 2 * odd + core, (other, z + core * across), (other, z + (1 - core) * across)


def regroup(count_dp):
    moves = []
    for dp in range(count_dp):
        for c in range(4):
            to = (dp - dp % 2 + c % 2) * 4 + 2 * (dp % 2) + c // 2
            moves.append((dp * 4 + c, to))
    return moves


def mm(x, w):
    return jnp.dot(x, w, preferred_element_type=F32)


def mm_nt(x, w):
    return lax.dot_general(x, w, (((1,), (1,)), ((), ())), preferred_element_type=F32)


def mm_tn(x, w):
    return lax.dot_general(x, w, (((0,), (0,)), ((), ())), preferred_element_type=F32)


def row_mean(values):
    return jnp.mean(values, axis=-1, keepdims=True)


def norm_forward(entry):
    centered = entry - row_mean(entry)
    scale = lax.rsqrt(row_mean(centered * centered) + 1e-05)
    return centered * scale, scale


def norm_backward(grad, gain, unit, scale):
    e = grad * gain
    return (e - row_mean(e) - unit * row_mean(e * unit)) * scale


def split_pair(pair):
    lane = lax.broadcasted_iota(jnp.int32, pair.shape, 1)
    zero = jnp.zeros_like(pair)
    return jnp.concatenate([jnp.where(lane < 64, pair, zero), jnp.where(lane < 64, zero, pair)], axis=0)


def join_pair(both):
    half = both.shape[0] // 2
    lane = lax.broadcasted_iota(jnp.int32, (half, 128), 1)
    return jnp.where(lane < 64, both[:half], both[half:])


def block_kernel(
    a_hbm, b_hbm, tok_ref, cot_ref, ids_ref,
    act_ref, ig_ref, ga_hbm, gb_hbm,
    wa, wb, small, cur, mid, kv, dkv, ids_got, bias_t,
    normed_s, unit1, scale1, q_s, att_s, unit2, scale2, nm_s, slope_s, actv_s, lse_s,
    branch_s, hg_s, aog_s, pg_s, qbd, dobd, delta_s, m_s, l_s, acc_s, sums,
    far_out, near_out, far_in, near_in, stage,
    wsem, isem, fsend, frecv, bsend, brecv, gsem,
):
    chunk, nxt, prv = ring()
    T = tok_ref.shape[0]
    D = tok_ref.shape[1]
    R = cot_ref.shape[0]
    FF = wb.shape[0]
    pairs = D // 128
    S = 3 * T
    q_cols, kv_cols = pl.ds(0, D), pl.ds(D, 2 * D)
    out_cols = pl.ds(3 * D, D)
    up0 = 4 * D
    small0 = up0 + FF

    barrier = pltpu.get_barrier_semaphore()
    for peer in (nxt, prv):
        pl.semaphore_signal(barrier, inc=1, device_id=peer, device_id_type=MESH)
    parts = (
        (a_hbm.at[:, pl.ds(small0, 128)], wa.at[:, pl.ds(small0, 128)]),
        (a_hbm.at[:, pl.ds(0, 3 * D)], wa.at[:, pl.ds(0, 3 * D)]),
        (a_hbm.at[:, out_cols], wa.at[:, out_cols]),
        (a_hbm.at[:, pl.ds(up0, FF)], wa.at[:, pl.ds(up0, FF)]),
        (b_hbm, wb),
    )
    fetch = [pltpu.make_async_copy(src, dst, wsem.at[n]) for n, (src, dst) in enumerate(parts)]
    for copy in fetch:
        copy.start()
    pl.semaphore_wait(barrier, 2)

    def remote(src, dst, send_sem, recv_sem, to):
        return pltpu.make_async_remote_copy(
            src_ref=src, dst_ref=dst, send_sem=send_sem, recv_sem=recv_sem, device_id=to, device_id_type=MESH
        )

    first_ids = remote(ids_ref.at[pl.ds(1, 2)], ids_got.at[pl.ds(0, 2)], isem.at[0], isem.at[1], nxt)
    first_ids.start()
    cur[...] = tok_ref[...].astype(F32)
    sums[...] = jnp.zeros_like(sums)
    fetch[0].wait()
    small[...] = jnp.transpose(wa[:, pl.ds(small0, 128)].astype(F32))

    @pl.loop(0, R * 3)
    def _(step):
        dkv[pl.ds(pl.multiple_of(step * T, T), T), :] = jnp.zeros((T, 2 * D), F32)

    first_ids.wait()
    second_ids = remote(ids_got.at[1], ids_got.at[2], isem.at[2], isem.at[3], nxt)
    second_ids.start()
    second_ids.wait()
    key_row = ids_ref[0, 0:1, :] + ids_got[0, 0:1, :] + ids_got[2, 0:1, :]
    own_row = ids_ref[0, 0:1, 0:128] + ids_ref[1, 0:1, 0:128]
    own_col = jnp.transpose(jnp.broadcast_to(own_row, (128, 128)))[:, 0:1]
    shape = (2 * T, 4 * T)
    key = lax.broadcasted_iota(jnp.int32, shape, 1)
    query = lax.broadcasted_iota(jnp.int32, shape, 0)
    query = jnp.where(query >= T, query - T, query)
    slot = key // T
    allowed = (jnp.broadcast_to(key_row, shape) == jnp.broadcast_to(own_col, shape)) & (slot < 3)
    allowed = allowed & (slot <= chunk) & ((slot > 0) | (key <= query))
    full_bias = jnp.where(allowed, 0.0, -1e30).astype(F32)
    bias_t[...] = jnp.transpose(full_bias)

    def small_row(index):
        return small[pl.ds(index, 1), :]

    def rows(r):
        return pl.ds(pl.multiple_of(r * T, T), T)

    def keys(r, first, count):
        return pl.ds(pl.multiple_of(r * S + first * T, T), count * T)

    def kv_copies(r):
        own, near, far = keys(r, 0, 1), keys(r, 1, 1), keys(r, 2, 1)
        return (
            remote(kv.at[own], kv.at[near], fsend.at[0, r], frecv.at[0, r], nxt),
            remote(kv.at[near], kv.at[far], fsend.at[1, r], frecv.at[1, r], nxt),
        )

    def attend(row_slice, slots):
        for p in range(pairs):
            cols = pl.ds(p * 128, 128)
            values = pl.ds(D + p * 128, 128)
            scores = mm_nt(kv[row_slice, cols], qbd[cols, :]) + bias_t[slots, :]
            old = m_s[0:1, cols]
            new = jnp.maximum(old, jnp.max(scores, axis=0, keepdims=True))
            weight = jnp.exp(scores - new)
            shrink = jnp.exp(old - new)
            m_s[0:1, cols] = new
            l_s[0:1, cols] = l_s[0:1, cols] * shrink + jnp.sum(weight, axis=0, keepdims=True)
            acc_s[cols, :] = acc_s[cols, :] * shrink + mm_tn(kv[row_slice, values], weight.astype(BF16))

    def forward(r, carry):
        mine = rows(r)
        first, second = kv_copies(r)
        entry = cur[...] + small_row(4 + r)
        unit, scale = norm_forward(entry)
        unit1[mine, :] = unit
        scale1[mine, :] = jnp.broadcast_to(scale, (T, 128))
        normed = (unit * small_row(0) + small_row(1)).astype(BF16)
        normed_s[mine, :] = normed

        @pl.when(r == 0)
        def _():
            fetch[1].wait()

        kv[keys(r, 0, 1), :] = mm(normed, wa[:, kv_cols]).astype(BF16)
        first.start()
        queries = mm(normed, wa[:, q_cols]).astype(BF16) * jnp.asarray(0.125, BF16)
        q_s[mine, :] = queries
        for p in range(pairs):
            qbd[pl.ds(p * 128, 128), :] = split_pair(queries[:, p * 128 : p * 128 + 128])
        m_s[...] = jnp.full_like(m_s, -1e30)
        l_s[...] = jnp.zeros_like(l_s)
        acc_s[...] = jnp.zeros_like(acc_s)
        lax.fori_loop(0, r, lambda e, c: (attend(keys(e, 0, 3), pl.ds(0, S)), c)[1], 0)
        attend(keys(r, 0, 1), pl.ds(0, T))
        first.wait_recv()
        second.start()
        attend(keys(r, 1, 1), pl.ds(T, T))
        second.wait_recv()
        attend(keys(r, 2, 1), pl.ds(2 * T, T))
        for p in range(pairs):
            cols = pl.ds(p * 128, 128)
            att_s[mine, cols] = join_pair(jnp.transpose(acc_s[cols, :] / l_s[0:1, cols])).astype(BF16)
        lse_s[pl.ds(pl.multiple_of(r * 8, 8), 8), :] = jnp.broadcast_to(m_s[0:1, :] + jnp.log(l_s[0:1, :]), (8, D))

        @pl.when(r == 0)
        def _():
            fetch[2].wait()

        middle = entry + mm(att_s[mine, :], wa[:, out_cols])
        unit, scale = norm_forward(middle)
        unit2[mine, :] = unit
        scale2[mine, :] = jnp.broadcast_to(scale, (T, 128))
        normed = (unit * small_row(2) + small_row(3)).astype(BF16)
        nm_s[mine, :] = normed

        @pl.when(r == 0)
        def _():
            fetch[3].wait()
            fetch[4].wait()

        total = middle
        for j in range(FF // D):
            hidden = mm(normed, wa[:, pl.ds(up0 + j * D, D)])
            square = hidden * hidden
            root = 0.7978845608028654
            t = jnp.tanh(root * hidden * (1.0 + 0.044715 * square))
            slope_s[mine, pl.ds(j * D, D)] = 0.5 * (1.0 + t) + 0.5 * root * hidden * (1.0 - t * t) * (
                1.0 + 3 * 0.044715 * square
            )
            activated = (0.5 * hidden * (1.0 + t)).astype(BF16)
            actv_s[mine, pl.ds(j * D, D)] = activated
            total = total + mm(activated, wb[pl.ds(j * D, D), :])
        cur[...] = total
        act_ref[r] = total.astype(BF16)
        first.wait_send()
        second.wait_send()
        return carry

    lax.fori_loop(0, R, forward, 0)
    cur[...] = jnp.zeros_like(cur)

    def grad_block(e):
        block = keys(e, 0, 3)
        for p in range(pairs):
            cols = pl.ds(p * 128, 128)
            state = pl.ds(p * 128, 128)
            values = pl.ds(D + p * 128, 128)
            k_pair, v_pair = kv[block, cols], kv[block, values]
            q_pair, o_pair = qbd[state, :], dobd[state, :]
            scores = mm_nt(k_pair, q_pair) + bias_t[0:S, :]
            probs = jnp.exp(scores - delta_s[0:1, cols])
            grad = probs * (mm_nt(v_pair, o_pair) - delta_s[8:9, cols])
            low = grad.astype(BF16)
            dkv[block, cols] += mm(low, q_pair)
            dkv[block, values] += mm(probs.astype(BF16), o_pair)
            acc_s[state, :] += mm_tn(low, k_pair)

    def backward(i, carry):
        r = R - 1 - i
        mine = rows(r)
        grad_out = cot_ref[r].astype(F32) + cur[...]
        branch = grad_out.astype(BF16)
        branch_s[mine, :] = branch
        e = jnp.zeros((T, D), F32)
        for j in range(FF // D):
            part = pl.ds(j * D, D)
            low = (mm_nt(branch, wb[part, :]) * slope_s[mine, part]).astype(BF16)
            hg_s[mine, part] = low
            e = e + mm_nt(low, wa[:, pl.ds(up0 + j * D, D)])
        unit = unit2[mine, :]
        sums[2:3, :] += jnp.sum(e * unit, axis=0, keepdims=True)
        sums[3:4, :] += jnp.sum(e, axis=0, keepdims=True)
        middle_grad = grad_out + norm_backward(e, small_row(2), unit, scale2[mine, 0:1])
        mid[...] = middle_grad
        low = middle_grad.astype(BF16)
        aog_s[mine, :] = low
        mixed = mm_nt(low, wa[:, out_cols]).astype(BF16)
        queries = q_s[mine, :]
        attended = att_s[mine, :]
        for p in range(pairs):
            state = pl.ds(p * 128, 128)
            lo, hi = p * 128, p * 128 + 128
            qbd[state, :] = split_pair(queries[:, lo:hi])
            o_pair = split_pair(mixed[:, lo:hi])
            dobd[state, :] = o_pair
            twice = jnp.concatenate([attended[:, lo:hi], attended[:, lo:hi]], axis=0)
            product = jnp.transpose(o_pair.astype(F32) * twice.astype(F32))
            delta_s[8:16, lo:hi] = jnp.broadcast_to(jnp.sum(product, axis=0, keepdims=True), (8, 128))
        delta_s[0:8, :] = lse_s[pl.ds(pl.multiple_of(r * 8, 8), 8), :]
        acc_s[...] = jnp.zeros_like(acc_s)
        grad_block(r)
        far_out[r] = dkv[keys(r, 2, 1), :].astype(BF16)
        far = remote(far_out.at[r], far_in.at[r], bsend.at[0, r], brecv.at[0, r], prv)
        far.start()
        lax.fori_loop(0, r, lambda e, c: (grad_block(e), c)[1], 0)
        far.wait_recv()
        near_out[r] = (dkv[keys(r, 1, 1), :] + far_in[r].astype(F32)).astype(BF16)
        near = remote(near_out.at[r], near_in.at[r], bsend.at[1, r], brecv.at[1, r], prv)
        near.start()
        for p in range(pairs):
            pg_s[mine, pl.ds(p * 128, 128)] = (0.125 * join_pair(acc_s[pl.ds(p * 128, 128), :])).astype(BF16)
        e = mm_nt(pg_s[mine, q_cols], wa[:, q_cols])
        near.wait_recv()
        low = (dkv[keys(r, 0, 1), :] + near_in[r].astype(F32)).astype(BF16)
        pg_s[mine, kv_cols] = low
        e = e + mm_nt(low, wa[:, kv_cols])
        unit = unit1[mine, :]
        sums[0:1, :] += jnp.sum(e * unit, axis=0, keepdims=True)
        sums[1:2, :] += jnp.sum(e, axis=0, keepdims=True)
        entry_grad = mid[...] + norm_backward(e, small_row(0), unit, scale1[mine, 0:1])
        cur[...] = entry_grad
        sums[pl.ds(4 + r, 1), :] = jnp.sum(entry_grad, axis=0, keepdims=True)
        far.wait_send()
        near.wait_send()
        return carry

    lax.fori_loop(0, R, backward, 0)
    ig_ref[...] = cur[...]

    wa[:, pl.ds(small0, 128)] = jnp.transpose(sums[...]).astype(BF16)
    tail = pltpu.make_async_copy(wa.at[:, pl.ds(small0, 128)], ga_hbm.at[:, pl.ds(small0, 128)], wsem.at[0])
    tail.start()

    def piece(n, features, grads, target):
        hold = n % 2 if isinstance(n, int) else lax.rem(n, 2)
        copy = pltpu.make_async_copy(stage.at[hold], target, gsem.at[hold])
        if not (isinstance(n, int) and n < 2):
            @pl.when(n >= 2)
            def _():
                copy.wait()

        stage[hold] = mm_tn(features, grads).astype(BF16)
        copy.start()

    def wide(n0, count, feature_ref, grad_ref, col0):
        def body(j, c):
            part = pl.ds(pl.multiple_of(j * D, D), D)
            piece(n0 + j, feature_ref[...], grad_ref[:, part], ga_hbm.at[:, pl.ds(pl.multiple_of(col0 + j * D, D), D)])
            return c

        lax.fori_loop(0, count, body, 0)

    wide(0, 3, normed_s, pg_s, 0)
    wide(3, 1, att_s, aog_s, 3 * D)
    wide(4, FF // D, nm_s, hg_s, up0)

    def tall(j, c):
        part = pl.ds(pl.multiple_of(j * D, D), D)
        piece(4 + FF // D + j, actv_s[:, part], branch_s[...], gb_hbm.at[part, :])
        return c

    lax.fori_loop(0, FF // D, tall, 0)
    for hold in (0, 1):
        pltpu.make_async_copy(stage.at[hold], gb_hbm.at[pl.ds(0, D), :], gsem.at[hold]).wait()
    tail.wait()


def run_block(all_a, all_b, tokens, cot, ids):
    T, D = tokens.shape
    R = cot.shape[0]
    FF = all_b.shape[0]
    rows = R * T
    V = pltpu.VMEM
    DMA = pltpu.SemaphoreType.DMA
    return pl.pallas_call(
        block_kernel,
        out_shape=(
            jax.ShapeDtypeStruct((R, T, D), BF16),
            jax.ShapeDtypeStruct((T, D), F32),
            jax.ShapeDtypeStruct(all_a.shape, BF16),
            jax.ShapeDtypeStruct(all_b.shape, BF16),
        ),
        in_specs=[pl.BlockSpec(memory_space=pl.ANY)] * 2 + [pl.BlockSpec(memory_space=pltpu.VMEM)] * 3,
        out_specs=[pl.BlockSpec(memory_space=pltpu.VMEM)] * 2 + [pl.BlockSpec(memory_space=pl.ANY)] * 2,
        scratch_shapes=[
            V(all_a.shape, BF16), V(all_b.shape, BF16), V((128, D), F32), V((T, D), F32), V((T, D), F32),
            V((3 * rows, 2 * D), BF16), V((3 * rows, 2 * D), F32), V((3, 8, 256), F32),
            V((256, 128), F32),
            V((rows, D), BF16), V((rows, D), F32), V((rows, 128), F32), V((rows, D), BF16), V((rows, D), BF16),
            V((rows, D), F32), V((rows, 128), F32), V((rows, D), BF16), V((rows, FF), F32), V((rows, FF), BF16),
            V((8 * R, D), F32),
            V((rows, D), BF16), V((rows, FF), BF16), V((rows, D), BF16), V((rows, 3 * D), BF16),
            V((D, 128), BF16), V((D, 128), BF16), V((16, D), F32), V((8, D), F32), V((8, D), F32), V((D, 128), F32),
            V((128, D), F32),
            V((R, T, 2 * D), BF16), V((R, T, 2 * D), BF16), V((R, T, 2 * D), BF16), V((R, T, 2 * D), BF16),
            V((2, D, D), BF16),
            DMA((5,)), DMA((4,)), DMA((2, R)), DMA((2, R)), DMA((2, R)), DMA((2, R)), DMA((2,)),
        ],
        compiler_params=pltpu.CompilerParams(
            collective_id=2, has_side_effects=True, vmem_limit_bytes=VMEM_LIMIT
        ),
    )(all_a, all_b, tokens, cot, ids)


def on_device(
    tokens,
    qkv_weight,
    out_weight,
    up_weight,
    down_weight,
    attn_gain,
    attn_shift,
    ffn_gain,
    ffn_shift,
    pass_embed,
    segment_ids,
    cotangent,
):
    _, local_tok, model_width = tokens.shape
    repeats = pass_embed.shape[0]
    qkv_cols, ff_width = qkv_weight.shape[1], up_weight.shape[1]
    small_in = jnp.stack([attn_gain, attn_shift, ffn_gain, ffn_shift], axis=1)
    small_in = jnp.concatenate([small_in, pass_embed.T], axis=1)
    small_in = jnp.pad(small_in, ((0, 0), (0, 128 - small_in.shape[1])))
    rows_a = jnp.concatenate([qkv_weight, out_weight, up_weight, small_in], axis=1)
    block_of_slice = (lax.axis_size("dp"), lax.axis_size("ctx")) == (8, 4)
    if block_of_slice:
        all_a, all_b = gather_blocks(rows_a, down_weight)
    else:
        all_a = lax.all_gather(rows_a, ("dp", "ctx"), axis=0)
        all_b = lax.all_gather(down_weight, ("dp", "ctx"), axis=0)
    all_a = all_a.reshape(model_width, -1)
    all_b = all_b.reshape(-1, model_width)
    moves = regroup(lax.axis_size("dp"))
    back = [(to, came) for came, to in moves]
    axes = ("dp", "ctx")
    own_ids = lax.ppermute(segment_ids, axes, moves).astype(F32)
    tokens = lax.ppermute(tokens, axes, moves)
    cotangent = lax.ppermute(cotangent, axes, moves)
    ids = jnp.stack([jnp.pad(own_ids, ((0, 0), (s * local_tok, (3 - s) * local_tok))) for s in range(3)])
    ids = jnp.broadcast_to(ids, (3, 8, 4 * local_tok))
    cot = cotangent.reshape(local_tok, repeats, model_width).transpose(1, 0, 2)
    outputs, input_grad, grad_a, grad_b = run_block(all_a, all_b, tokens[0], cot, ids)
    grad_a = grad_a.reshape(-1, *rows_a.shape)
    grad_b = grad_b.reshape(-1, *down_weight.shape)
    if block_of_slice:
        own_a, own_b = reduce_blocks(grad_a, grad_b)
    else:
        own_a = lax.psum_scatter(grad_a.astype(F32), ("dp", "ctx"), scatter_dimension=0)
        own_b = lax.psum_scatter(grad_b.astype(F32), ("dp", "ctx"), scatter_dimension=0)
    own_small = own_a[:, qkv_cols + model_width + ff_width :].T
    outputs = lax.ppermute(outputs, axes, back)
    input_grad = lax.ppermute(input_grad, axes, back)
    activations = outputs.transpose(1, 0, 2).reshape(1, local_tok * repeats, model_width)
    return (
        activations,
        input_grad[None],
        own_a[:, :qkv_cols],
        own_a[:, qkv_cols : qkv_cols + model_width],
        own_a[:, qkv_cols + model_width : qkv_cols + model_width + ff_width],
        own_b,
        own_small[0],
        own_small[1],
        own_small[2],
        own_small[3],
        own_small[4 : 4 + repeats],
    )


def solution(mesh):
    return jax.shard_map(
        on_device,
        mesh=mesh,
        in_specs=(
            P("dp", "ctx", None),
            P(("dp", "ctx"), None),
            P(("dp", "ctx"), None),
            P(("dp", "ctx"), None),
            P(("dp", "ctx"), None),
            P(("dp", "ctx")),
            P(("dp", "ctx")),
            P(("dp", "ctx")),
            P(("dp", "ctx")),
            P(None, ("dp", "ctx")),
            P("dp", "ctx"),
            P("dp", "ctx", None),
        ),
        out_specs=(
            P("dp", "ctx", None),
            P("dp", "ctx", None),
            P(("dp", "ctx"), None),
            P(("dp", "ctx"), None),
            P(("dp", "ctx"), None),
            P(("dp", "ctx"), None),
            P(("dp", "ctx")),
            P(("dp", "ctx")),
            P(("dp", "ctx")),
            P(("dp", "ctx")),
            P(None, ("dp", "ctx")),
        ),
        check_vma=False,
    )
```
